32 devices in a mesh: tp: 4 (over z), dp: 8 (over y, x, core).
Axes of the slice: x: 2, y: 2, z: 4, core: 2. Of those that a mesh axis runs over, the one named last changes fastest.
Arguments:
- w_in: float32 [2, 1024, 7168], P(None, None, 'tp')
- w_out: float32 [2, 5120, 1024], P(None, 'tp')
- g_in: float32 [8, 2, 1024, 7168], P('dp', None, None, 'tp')
- g_out: float32 [8, 2, 5120, 1024], P('dp', None, 'tp')
- m_in: bfloat16 [2, 1024, 7168], P(None, 'dp', 'tp')
- m_out: bfloat16 [2, 5120, 1024], P(None, 'tp', 'dp')
- r_in: float32 [2, 1024], P(None, 'dp')
- c_in: float32 [2, 7168], P(None, 'tp')
- r_out: float32 [2, 5120], P(None, 'tp')
- c_out: float32 [2, 1024], P(None, 'dp')
- learn_rate: float32 [], replicated
- weight_decay: float32 [], replicated
- beta_two: float32 [], replicated
Outputs:
- output 1: float32 [2, 1024, 7168], P(None, None, 'tp')
- output 2: float32 [2, 5120, 1024], P(None, 'tp')
- output 3: bfloat16 [2, 1024, 7168], P(None, 'dp', 'tp')
- output 4: bfloat16 [2, 5120, 1024], P(None, 'tp', 'dp')
- output 5: float32 [2, 1024], P(None, 'dp')
- output 6: float32 [2, 7168], P(None, 'tp')
- output 7: float32 [2, 5120], P(None, 'tp')
- output 8: float32 [2, 1024], P(None, 'dp')
All inputs are finite; a program needn't handle non-finite values.
Results may differ from the reference program's by a relative error of at most 0.00121581.
Values sent between devices are 32-bit elements.
A program may use at most 1 GiB of HBM per device.

```python
import math
import jax
import jax.numpy as jnp

LAYERS = 2
D = 1024
MLP = 4096
DP = 8

FIN = MLP + 3 * D
FOUT = MLP + D


def axis_scales(key, count):
    key_ramp, key_noise = jax.random.split(key)
    ramp_slope = jax.random.uniform(key_ramp, (LAYERS, 1), jnp.float32, 0.6, 1.0)
    ramp_vals = jnp.linspace(-1.0, 1.0, count, dtype=jnp.float32)[None, :]
    noise_vals = jax.random.normal(key_noise, (LAYERS, count), jnp.float32)
    return jnp.exp(ramp_slope * ramp_vals + 0.3 * noise_vals)


def draw_matrix(key, n_rows, n_cols):
    key_list = jax.random.split(key, 7)
    row_scale = axis_scales(key_list[0], n_rows)
    col_scale = axis_scales(key_list[1], n_cols)
    noise_rep = jax.random.normal(key_list[2], (DP, LAYERS, n_rows, n_cols), jnp.float32)
    grad_rep = noise_rep * (row_scale[:, :, None] * col_scale[:, None, :] / math.sqrt(DP))
    grad_sum = jnp.sum(grad_rep, axis=0)
    grad_sq = grad_sum * grad_sum
    row_noise = jax.random.normal(key_list[3], (LAYERS, n_rows), jnp.float32)
    col_noise = jax.random.normal(key_list[4], (LAYERS, n_cols), jnp.float32)
    row_old = 0.25 * jnp.mean(grad_sq, axis=2) * jnp.exp(0.5 * row_noise)
    col_old = 0.25 * jnp.mean(grad_sq, axis=1) * jnp.exp(0.5 * col_noise)
    weight = jax.random.normal(key_list[5], (LAYERS, n_rows, n_cols), jnp.float32) * n_rows ** -0.5
    moment = (0.1 * jax.random.normal(key_list[6], (LAYERS, n_rows, n_cols), jnp.float32)).astype(jnp.bfloat16)
    return weight, grad_rep, moment, row_old, col_old


def setup_inputs(seed: int = 0) -> dict:
    key_list = jax.random.split(jax.random.key(seed), 5)
    w_in, g_in, m_in, r_in, c_in = draw_matrix(key_list[0], D, FIN)
    w_out, g_out, m_out, r_out, c_out = draw_matrix(key_list[1], FOUT, D)
    learn_rate = jax.random.uniform(key_list[2], (), jnp.float32, 0.25, 0.75) * D ** -0.5
    weight_decay = jax.random.uniform(key_list[3], (), jnp.float32, 0.15, 0.45) * D ** 0.5
    beta_two = jax.random.uniform(key_list[4], (), jnp.float32, 0.8, 0.9)
    return dict(w_in=w_in, w_out=w_out, g_in=g_in, g_out=g_out, m_in=m_in, m_out=m_out, r_in=r_in, c_in=c_in, r_out=r_out, c_out=c_out, learn_rate=learn_rate, weight_decay=weight_decay, beta_two=beta_two)


def adafactor_matrix(weight, grad_rep, moment, row_old, col_old, learn_rate, weight_decay, beta_two):
    grad_sum = jnp.sum(grad_rep, axis=0)
    grad_sq = grad_sum * grad_sum + 1e-30
    row_new = beta_two * row_old + (1.0 - beta_two) * jnp.mean(grad_sq, axis=2)
    col_new = beta_two * col_old + (1.0 - beta_two) * jnp.mean(grad_sq, axis=1)
    row_avg = jnp.mean(row_new, axis=1)
    second = row_new[:, :, None] * col_new[:, None, :] / row_avg[:, None, None]
    update = grad_sum / jnp.sqrt(second)
    rms_val = jnp.sqrt(jnp.mean(update * update, axis=(1, 2)))
    update = update / jnp.maximum(1.0, rms_val)[:, None, None]
    mom_new = (0.9 * moment.astype(jnp.float32) + 0.1 * update).astype(jnp.bfloat16)
    w_new = weight - learn_rate * mom_new.astype(jnp.float32) - learn_rate * weight_decay * weight
    return w_new, mom_new, row_new, col_new


def reference(w_in, w_out, g_in, g_out, m_in, m_out, r_in, c_in, r_out, c_out, learn_rate, weight_decay, beta_two):
    in_result = adafactor_matrix(w_in, g_in, m_in, r_in, c_in, learn_rate, weight_decay, beta_two)
    out_result = adafactor_matrix(w_out, g_out, m_out, r_out, c_out, learn_rate, weight_decay, beta_two)
    return (in_result[0], out_result[0], in_result[1], out_result[1], in_result[2], in_result[3], out_result[2], out_result[3])
```

```python
import jax
import jax.numpy as jnp
from jax import lax
from jax.experimental import pallas as pl
from jax.experimental.pallas import tpu as pltpu
from jax.sharding import PartitionSpec as P

MESH = pl.DeviceIdType.MESH
F32 = jnp.float32
LANES = 128
TP, DP = 4, 8
PARTS = 4
STORES = 4


def total(x):
    return jnp.sum(jnp.sum(x, axis=0, keepdims=True), axis=1, keepdims=True)


def eye_mask():
    row = lax.broadcasted_iota(jnp.int32, (LANES, LANES), 0)
    col = lax.broadcasted_iota(jnp.int32, (LANES, LANES), 1)
    return row == col


def to_row(col):
    return jnp.sum(jnp.where(eye_mask(), jnp.broadcast_to(col, (LANES, LANES)), 0.0), axis=0, keepdims=True)


def to_rows(row):
    col = jnp.sum(jnp.where(eye_mask(), jnp.broadcast_to(row, (LANES, LANES)), 0.0), axis=1, keepdims=True)
    return jnp.broadcast_to(col, (LANES, LANES))


def fused_kernel(g_in, g_out, w_in, w_out, m_in, m_out, r_in, c_in, r_out, c_out, lr_ref, wd_ref, b2_ref,
                 ow_in, ow_out, om_in, om_out, or_in, oc_in, or_out, oc_out,
                 gm_in, gm_out, r1_in, r1_out, r2_in, r2_out, ws_in, ws_out,
                 vr_in, vc_in, vr_out, vc_out, vp_in, vp_out, vh_in, vh_out, vf_in, vf_out, ts, tr, rp, rc, short, olds, rb,
                 ld_sem, pre_sem, st_sem, sm_sem, d2_send, d2_first, d2_recv, p1_send, p1_recv, p2_send, p2_recv,
                 a_send, a1_recv, a2_recv, a2_last, ad_send, ad_recv, v_send, v_recv, z_sem):
    t = lax.axis_index('tp')
    d = lax.axis_index('dp')
    core = lax.rem(d, 2)
    chip = d // 2
    x = lax.rem(chip, 2)
    y = chip // 2
    k_own = chip
    k_x = y * 2 + (1 - x)
    k_y = (1 - y) * 2 + x
    k_d = (1 - y) * 2 + (1 - x)
    dev_x = k_x * 2 + core
    dev_y = k_y * 2 + core
    dev_d = k_d * 2 + core
    dev_c = chip * 2 + (1 - core)
    lr = lr_ref[0]
    wd = wd_ref[0]
    b2 = b2_ref[0]
    n_layers = gm_in.shape[0]
    mats = [(0, i) for i in range(n_layers)] + [(1, i) for i in range(n_layers)]
    n_mats = len(mats)
    sw = gm_in.shape[2]
    half_in = sw // 2
    cols_in = gm_in.shape[3]
    rows_out = gm_out.shape[2]
    half_out = rows_out // 2

    def full_view(refs, mat, q, h, lead):
        kind, l = mat
        pre = (0,) if lead else ()
        if kind == 0:
            return refs[0].at[pre + (l, pl.ds(pl.multiple_of(q * sw + h * half_in, half_in), half_in), slice(None))]
        return refs[1].at[pre + (l, pl.ds(h * half_out, half_out), pl.ds(pl.multiple_of(q * LANES, LANES), LANES))]

    def full_shard(refs, mat, q):
        kind, l = mat
        if kind == 0:
            return refs[0].at[l, pl.ds(pl.multiple_of(q * sw, sw), sw), :]
        return refs[1].at[l, :, pl.ds(pl.multiple_of(q * LANES, LANES), LANES)]

    def half_view(refs, mat, k, h):
        kind, l = mat
        size = half_in if kind == 0 else half_out
        return refs[kind].at[l, k, pl.ds(h * size, size)]

    gs = (g_in, g_out)
    ows = (ow_in, ow_out)
    gms = (gm_in, gm_out)
    r1s = (r1_in, r1_out)
    r2s = (r2_in, r2_out)
    oms = (om_in, om_out)
    wss = (ws_in, ws_out)

    def remote(src, dst, send, recv, dev_t, dev_d):
        cp = pltpu.make_async_remote_copy(src_ref=src, dst_ref=dst, send_sem=send, recv_sem=recv,
                                          device_id=(dev_t, dev_d), device_id_type=MESH)
        cp.start()
        return cp

    def wait_bytes(ref, sem):
        pltpu.make_async_copy(ref, ref, sem).wait()

    def add_into(dst, src):
        rows, cols = dst.shape
        step = 8 if cols > LANES else 128
        if rows % step:
            step = 8

        def body(i, carry):
            sl = pl.ds(pl.multiple_of(i * step, step), step)
            dst[sl, :] = dst[sl, :] + src[sl, :]
            return carry

        lax.fori_loop(0, rows // step, body, 0)

    pieces = [(k_d, 0), (k_d, 1), (k_x, 0), (k_y, 1), (k_y, 0), (k_x, 1), (k_own, 0), (k_own, 1)]
    routes = [(0, 1, dev_x), (1, 1, dev_y), (0, 0, dev_x), (1, 0, dev_y)]

    def sub(ref, i):
        rows = ref.shape[0] // PARTS
        return ref.at[pl.ds(i * rows, rows)]

    def start_loads(m):
        mat = mats[m]
        for i, (k, h) in enumerate(pieces):
            sem = ld_sem.at[min(i, 2)] if m == 0 else ld_sem.at[2 + m]
            pltpu.make_async_copy(full_view(gs, mat, 2 * k + core, h, True), half_view(gms, mat, k, h), sem).start()

    def start_preload():
        for i, (k, h) in enumerate(pieces):
            q = 2 * k + (1 - core)
            pltpu.make_async_copy(full_view(gs, mats[0], q, h, True), full_view(ows, mats[0], q, h, False), pre_sem.at[min(i, 2)]).start()

    def swap_first():
        views = [full_view(ows, mats[0], 2 * k + (1 - core), h, False) for k, h in pieces]
        for i in range(2):
            wait_bytes(views[i], pre_sem.at[i])
            remote(sub(views[i], 0), sub(views[i], 0), d2_send.at[2], d2_first.at[i, 0], t, dev_c)
        for p in range(1, PARTS):
            for i in range(2):
                remote(sub(views[i], p), sub(views[i], p), d2_send.at[2], d2_first.at[i, p], t, dev_c)
        wait_bytes(gm_in.at[0, pl.ds(0, 3)], pre_sem.at[2])
        for i in range(2, 8):
            remote(views[i], views[i], d2_send.at[2], d2_recv.at[min(i - 2, 2)], t, dev_c)

    def start_swap(m):
        mat = mats[m]
        for k, h in pieces:
            q = 2 * k + (1 - core)
            remote(full_view(gs, mat, q, h, True), full_view(ows, mat, q, h, False), d2_send.at[mat[0]], d2_recv.at[2 + m], t, dev_c)

    def chip_views(m, i):
        k, h = pieces[i]
        return half_view(gms, mats[m], k, h), full_view(ows, mats[m], 2 * k + core, h, False)

    def send_first(m, i, part=None):
        kind, l = mats[m]
        h, j, dev = routes[i]
        mine, other = chip_views(m, i)
        dst = r1s[kind].at[l, h, j]
        if part is not None:
            mine, other, dst = sub(mine, part), sub(other, part), sub(dst, part)
        add_into(mine, other)
        remote(mine, dst, p1_send.at[kind], p1_recv.at[m, 2 * h + j], t, dev)

    def stage_a_first():
        views = [chip_views(0, i)[0] for i in range(8)]
        for i in range(2):
            wait_bytes(views[i], ld_sem.at[i])
        for p in range(PARTS):
            for i in range(2):
                wait_bytes(sub(views[i], p), d2_first.at[i, p])
                send_first(0, i, p)
        wait_bytes(gm_in.at[0, pl.ds(0, 3)], ld_sem.at[2])
        for i in range(2, 4):
            wait_bytes(views[i], d2_recv.at[i - 2])
            send_first(0, i)

    def keep_first(m):
        for i in range(4, 8):
            add_into(*chip_views(m, i))

    def stage_a(m):
        kind, l = mats[m]
        gm = gms[kind].at[l]
        wait_bytes(gm, ld_sem.at[2 + m])
        wait_bytes(gm, d2_recv.at[2 + m])
        for i in range(4):
            send_first(m, i)
        keep_first(m)

    def stage_b(m):
        kind, l = mats[m]
        for h, k, dev in ((0, k_y, dev_y), (1, k_x, dev_x)):
            mine = half_view(gms, mats[m], k, h)
            wait_bytes(mine, p1_recv.at[m, 2 * h + 1])
            add_into(mine, r1s[kind].at[l, h, 1])
            remote(mine, r2s[kind].at[l, h], p2_send.at[kind], p2_recv.at[m, h], t, dev)
        for h in range(2):
            mine = half_view(gms, mats[m], k_own, h)
            wait_bytes(mine, p1_recv.at[m, 2 * h])
            add_into(mine, r1s[kind].at[l, h, 0])

    vps = (vp_in, vp_out)
    vhs = (vh_in, vh_out)
    vfs = (vf_in, vf_out)

    def send_chips(slots, send, recv):
        for dev in (dev_x, dev_y, dev_d):
            remote(slots.at[chip], slots.at[chip], send, recv, t, dev)

    def send_core(slots, send, recv):
        remote(slots.at[core], slots.at[core], send, recv, t, dev_c)

    def send_tp(slots, send, recv):
        for i in range(1, TP):
            remote(slots.at[t], slots.at[t], send, recv, lax.rem(t + i, TP), d)

    def sum_slots(slots, count):
        acc = slots[0]
        for i in range(1, count):
            acc = acc + slots[i]
        return acc

    def stage_c(m):
        kind, l = mats[m]
        mat = mats[m]
        for h in range(2):
            mine = half_view(gms, mat, k_own, h)
            wait_bytes(mine, p2_recv.at[m, h])
            add_into(mine, r2s[kind].at[l, h])
        own = vps[kind].at[l, core]
        shard = gms[kind].at[l, k_own]
        if kind == 0:
            def body(i, acc):
                sl = pl.ds(pl.multiple_of(i * 8, 8), 8)
                g = shard[sl, :]
                s = g * g + 1e-30
                rb[sl, :] = jnp.broadcast_to(jnp.sum(s, axis=1, keepdims=True), (8, LANES))
                return acc + s

            acc = lax.fori_loop(0, sw // 8, body, jnp.zeros((8, cols_in), F32))
            own[:, pl.ds(0, cols_in)] = jnp.sum(acc, axis=0, keepdims=True)
            own[:, pl.ds(cols_in, LANES)] = vr_in[pl.ds(l, 1), :]
            spare = own.shape[1] - cols_in - LANES
            if spare:
                own[:, pl.ds(cols_in + LANES, spare)] = jnp.zeros((1, spare), F32)
            short[pl.ds(m, 1), :] = to_row(rb[pl.ds(0, LANES), 0:1])
        else:
            def body(i, acc):
                g = shard[pl.ds(pl.multiple_of(i * LANES, LANES), LANES), :]
                s = g * g + 1e-30
                own[:, pl.ds(pl.multiple_of(i * LANES, LANES), LANES)] = to_row(jnp.sum(s, axis=1, keepdims=True))
                return acc + jnp.sum(s, axis=0, keepdims=True)

            short[pl.ds(m, 1), :] = lax.fori_loop(0, rows_out // LANES, body, jnp.zeros((1, LANES), F32))
        send_core(vps[kind].at[l], v_send.at[kind], v_recv.at[m, 0])

    def stage_k(m):
        kind, l = mats[m]
        both = vps[kind].at[l]
        wait_bytes(both.at[0], v_recv.at[m, 0])
        size = vhs[kind].shape[3]
        half = pl.ds(pl.multiple_of(core * size, LANES), size)
        vhs[kind].at[l, chip][...] = both.at[0][:, half] + both.at[1][:, half]
        send_chips(vhs[kind].at[l], v_send.at[2 + kind], v_recv.at[m, 1])

    def stage_d(m):
        kind, l = mats[m]
        slots = vhs[kind].at[l]
        wait_bytes(slots.at[pl.ds(0, 3)], v_recv.at[m, 1])
        vfs[kind].at[l, core][...] = sum_slots(slots, 4)
        send_core(vfs[kind].at[l], v_send.at[4 + kind], v_recv.at[m, 2])

    in_rows, in_cols = sw * DP, cols_in * TP
    out_rows, out_cols = rows_out * TP, sw * DP

    def stage_l(m):
        kind, l = mats[m]
        both = vfs[kind].at[l]
        wait_bytes(both.at[0], v_recv.at[m, 2])
        acc = jnp.concatenate([both[0], both[1]], axis=1)
        own = ts.at[m, t]
        own[:, pl.ds(0, LANES)] = short[pl.ds(m, 1), :]
        if kind == 0:
            col_sum = acc[:, :cols_in]
            oc_in[pl.ds(l, 1), :] = b2 * vc_in[pl.ds(l, 1), :] + (1.0 - b2) * (col_sum / in_rows)
            plane = jnp.sum(col_sum, axis=1, keepdims=True)
            olds[pl.ds(l, 1), :] = acc[:, cols_in:cols_in + LANES]
        else:
            r_new = b2 * vr_out[pl.ds(l, 1), :] + (1.0 - b2) * (acc / out_cols)
            or_out[pl.ds(l, 1), :] = r_new
            plane = jnp.sum(r_new, axis=1, keepdims=True)
        own[:, pl.ds(LANES, LANES)] = jnp.broadcast_to(plane, (1, LANES))
        send_tp(ts.at[m], v_send.at[6], v_recv.at[m, 3])

    def stage_e(m):
        kind, l = mats[m]
        wait_bytes(ts.at[m, pl.ds(0, TP - 1)], v_recv.at[m, 3])
        acc = sum_slots(ts.at[m], TP)
        vec = acc[:, :LANES]
        tot = acc[:, LANES:LANES + 1]
        shard = gms[kind].at[l, k_own]
        if kind == 0:
            r_new = b2 * vr_in[pl.ds(l, 1), :] + (1.0 - b2) * (vec / in_cols)
            or_in[pl.ds(l, 1), :] = r_new
            old = jnp.sum(olds[pl.ds(l, 1), :], axis=1, keepdims=True)
            avg = (b2 * old + (1.0 - b2) * (tot / in_cols)) / in_rows
            rb[pl.ds(0, LANES), :] = to_rows(1.0 / jnp.sqrt(r_new))
            cj = jnp.sqrt(avg) / jnp.sqrt(oc_in[pl.ds(l, 1), :])

            def body(i, acc):
                sl = pl.ds(pl.multiple_of(i * 8, 8), 8)
                u = (shard[sl, :] * rb[sl, 0:1]) * cj
                shard[sl, :] = u
                return acc + u * u

            sq = lax.fori_loop(0, sw // 8, body, jnp.zeros((8, cols_in), F32))
        else:
            c_new = b2 * vc_out[pl.ds(l, 1), :] + (1.0 - b2) * (vec / out_rows)
            oc_out[pl.ds(l, 1), :] = c_new
            avg = tot / out_rows
            cj = jnp.sqrt(avg) / jnp.sqrt(c_new)

            def body(i, acc):
                sl = pl.ds(pl.multiple_of(i * LANES, LANES), LANES)
                ri = to_rows(1.0 / jnp.sqrt(or_out[pl.ds(l, 1), sl]))
                u = (shard[sl, :] * ri) * cj
                shard[sl, :] = u
                return acc + u * u

            sq = lax.fori_loop(0, rows_out // LANES, body, jnp.zeros((LANES, LANES), F32))
        tr.at[m, t][...] = jnp.broadcast_to(total(sq), (1, LANES))
        send_tp(tr.at[m], v_send.at[7], v_recv.at[m, 4])

    def stage_f(m):
        wait_bytes(tr.at[m, pl.ds(0, TP - 1)], v_recv.at[m, 4])
        rp.at[m, core][...] = sum_slots(tr.at[m], TP)
        send_core(rp.at[m], v_send.at[8], v_recv.at[m, 5])

    def stage_n(m):
        wait_bytes(rp.at[m, 0], v_recv.at[m, 5])
        rc.at[m, chip][...] = rp.at[m][0] + rp.at[m][1]
        send_chips(rc.at[m], v_send.at[9], v_recv.at[m, 6])

    def stage_g(m):
        mat = mats[m]
        kind, l = mat
        wait_bytes(rc.at[m, pl.ds(0, 3)], v_recv.at[m, 6])
        size = float(in_rows * in_cols if kind == 0 else out_rows * out_cols)
        rms = jnp.sqrt(sum_slots(rc.at[m], 4) / size)
        scale = (1.0 / jnp.maximum(1.0, rms))[:, 0:1]
        shard = gms[kind].at[l, k_own]
        mom = oms[kind].at[l]
        old = wss[kind].at[l]
        new = full_shard(ows, mat, d)
        if l == 0:
            wait_bytes(oms[kind], st_sem.at[kind, 0])
            wait_bytes(wss[kind], st_sem.at[kind, 1])
        step = 16 if kind == 0 else 128

        def body(i, carry):
            sl = pl.ds(pl.multiple_of(i * step, step), step)
            mn = (0.9 * mom[sl, :].astype(F32) + 0.1 * (shard[sl, :] * scale)).astype(jnp.bfloat16)
            mom[sl, :] = mn
            w = old[sl, :]
            new[sl, :] = w - lr * mn.astype(F32) - lr * wd * w
            return carry

        lax.fori_loop(0, shard.shape[0] // step, body, 0)
        q = d
        a = full_view(ows, mat, q, 0, False)
        b = full_view(ows, mat, q, 1, False)
        remote(a, a, a_send.at[kind], a1_recv.at[m, 0], t, dev_y)
        remote(b, b, a_send.at[kind], a1_recv.at[m, 1], t, dev_x)
        remote(a, a, a_send.at[kind], a2_recv.at[m, 0], t, dev_x)
        remote(b, b, a_send.at[kind], a2_recv.at[m, 1], t, dev_y)
        pass_core(m, new)

    def pass_core(m, view):
        kind = mats[m][0]
        remote(view, view, ad_send.at[kind], ad_recv.at[kind], t, dev_c)

    def stage_h(m):
        mat = mats[m]
        kind = mat[0]
        a = full_view(ows, mat, 2 * k_y + core, 0, False)
        b = full_view(ows, mat, 2 * k_x + core, 1, False)
        for i, (view, dev) in enumerate(((a, dev_x), (b, dev_y))):
            wait_bytes(view, a1_recv.at[m, i])
            if m < n_mats - 1:
                remote(view, view, a_send.at[kind], a2_recv.at[m, 2 + i], t, dev)
            else:
                for p in range(PARTS):
                    remote(sub(view, p), sub(view, p), a_send.at[kind], a2_last.at[i, p], t, dev)
        pass_core(m, a)
        pass_core(m, b)

    def stage_i(m):
        last = m == n_mats - 1
        for i, k, h in ((0, k_x, 0), (1, k_y, 1)):
            view = full_view(ows, mats[m], 2 * k + core, h, False)
            wait_bytes(view, a2_recv.at[m, i])
            pass_core(m, view)
        views = [full_view(ows, mats[m], 2 * k_d + core, h, False) for h in range(2)]
        if not last:
            for i in range(2):
                wait_bytes(views[i], a2_recv.at[m, 2 + i])
                pass_core(m, views[i])
        else:
            for p in range(PARTS):
                for i in range(2):
                    wait_bytes(sub(views[i], p), a2_last.at[i, p])
                    pass_core(m, sub(views[i], p))

    small = [(r_in, vr_in), (c_in, vc_in), (r_out, vr_out), (c_out, vc_out)]
    barrier = pltpu.get_barrier_semaphore()
    z_near = jnp.minimum(t, 1) + jnp.minimum(TP - 1 - t, 1)

    def signal_z(sem):
        @pl.when(t > 0)
        def _():
            pl.semaphore_signal(sem, inc=1, device_id=(t - 1, d), device_id_type=MESH)

        @pl.when(t < TP - 1)
        def _():
            pl.semaphore_signal(sem, inc=1, device_id=(t + 1, d), device_id_type=MESH)

    for dev in (dev_x, dev_y, dev_c):
        pl.semaphore_signal(barrier, inc=1, device_id=(t, dev), device_id_type=MESH)
    signal_z(barrier)
    start_preload()
    start_loads(0)
    pl.semaphore_wait(barrier, 3 + z_near)
    swap_first()
    stage_a_first()
    start_loads(1)
    start_swap(1)
    signal_z(z_sem.at[0])
    wait_bytes(gm_in.at[0, pl.ds(0, 2)], d2_recv.at[2])
    keep_first(0)
    stage_a(1)
    for i, (src, dst) in enumerate(small):
        pltpu.make_async_copy(src, dst, sm_sem.at[i]).start()
    for m, (kind, l) in enumerate(mats):
        pltpu.make_async_copy((m_in, m_out)[kind].at[l], oms[kind].at[l], st_sem.at[kind, 0]).start()
        src = w_in.at[l, pl.ds(pl.multiple_of(d * sw, sw), sw), :] if kind == 0 else w_out.at[l, :, pl.ds(pl.multiple_of(d * LANES, LANES), LANES)]
        pltpu.make_async_copy(src, wss[kind].at[l], st_sem.at[kind, 1]).start()
    wait_bytes(gm_in.at[0], d2_send.at[2])
    pl.semaphore_wait(z_sem.at[0], z_near)
    signal_z(z_sem.at[1])
    for i, (src, dst) in enumerate(small):
        wait_bytes(dst, sm_sem.at[i])
    order = 's2 b0 a2 s3 b1 c0 k0 a3 b2 c1 k1 d0 l0 e0 f0 n0 b3 c2 k2 g0 d1 l1 e1 f1 n1 c3 k3 d2 l2 h0 e2 f2 n2 g1 i0 d3 l3 e3 f3 n3 h1 g2 i1 h2 g3 i2 h3 i3'
    def stage_s(m):
        start_loads(m)
        start_swap(m)

    stages = dict(s=stage_s, a=stage_a, b=stage_b, c=stage_c, d=stage_d, e=stage_e, f=stage_f, g=stage_g, h=stage_h, i=stage_i, k=stage_k, l=stage_l, n=stage_n)
    pl.semaphore_wait(z_sem.at[1], z_near)
    for item in order.split():
        stages[item[0]](int(item[1]))
    for kind in range(2):
        gm = gms[kind]
        wait_bytes(gm, ad_recv.at[kind])
        wait_bytes(gm.at[pl.ds(0, n_layers - 1 + kind)], d2_send.at[kind])
        wait_bytes(r1s[kind], p1_send.at[kind])
        wait_bytes(r2s[kind], p2_send.at[kind])
        wait_bytes(gm.at[:, pl.ds(0, 3)], a_send.at[kind])
        wait_bytes(gm, ad_send.at[kind])
        wait_bytes(vps[kind].at[pl.ds(0, n_layers), 0], v_send.at[kind])
        wait_bytes(vhs[kind].at[pl.ds(0, n_layers), pl.ds(0, 3)], v_send.at[2 + kind])
        wait_bytes(vfs[kind].at[pl.ds(0, n_layers), 0], v_send.at[4 + kind])
    wait_bytes(ts.at[pl.ds(0, n_mats), pl.ds(0, TP - 1)], v_send.at[6])
    wait_bytes(tr.at[pl.ds(0, n_mats), pl.ds(0, TP - 1)], v_send.at[7])
    wait_bytes(rp.at[pl.ds(0, n_mats), 0], v_send.at[8])
    wait_bytes(rc.at[pl.ds(0, n_mats), pl.ds(0, 3)], v_send.at[9])


def store_kernel(*refs):
    n = (len(refs) - 1) // 2
    sems = refs[-1]
    for i in range(n):
        src, dst = refs[i], refs[n + i]
        if i < 2:
            rows = src.shape[1] // STORES
            for l in range(src.shape[0]):
                for c in range(STORES):
                    pltpu.make_async_copy(src.at[l, pl.ds(c * rows, rows)], dst.at[l, pl.ds(c * rows, rows)], sems.at[i]).start()
        else:
            pltpu.make_async_copy(src, dst, sems.at[i]).start()
    for i in range(n):
        pltpu.make_async_copy(refs[i], refs[n + i], sems.at[i]).wait()


def local_step(w_in, w_out, g_in, g_out, m_in, m_out, r_in, c_in, r_out, c_out, lr, wd, b2):
    n_l, rows_in, cols_in = w_in.shape
    rows_out = w_out.shape[1]
    sw = rows_in // DP
    n_m = 2 * n_l
    vec = (cols_in + LANES + 2 * LANES - 1) // (2 * LANES) * (2 * LANES)
    hbm = pl.BlockSpec(memory_space=pltpu.HBM)
    vmem = pl.BlockSpec(memory_space=pltpu.VMEM)
    smem = pl.BlockSpec(memory_space=pltpu.SMEM)
    vm = pltpu.VMEM
    sem = pltpu.SemaphoreType.DMA
    outs = (w_in, w_out, m_in, m_out, r_in, c_in, r_out, c_out)
    res = pl.pallas_call(
        fused_kernel,
        out_shape=tuple(vm(a.shape, a.dtype) for a in outs),
        in_specs=[hbm] * 10 + [smem] * 3,
        out_specs=[vmem] * 8,
        scratch_shapes=[
            vm((n_l, 4, sw, cols_in), F32), vm((n_l, 4, rows_out, LANES), F32),
            vm((n_l, 2, 2, sw // 2, cols_in), F32), vm((n_l, 2, 2, rows_out // 2, LANES), F32),
            vm((n_l, 2, sw // 2, cols_in), F32), vm((n_l, 2, rows_out // 2, LANES), F32),
            vm((n_l, sw, cols_in), F32), vm((n_l, rows_out, LANES), F32),
            vm(r_in.shape, F32), vm(c_in.shape, F32), vm(r_out.shape, F32), vm(c_out.shape, F32),
            vm((n_l + 1, 2, 1, vec), F32), vm((n_l + 1, 2, 1, rows_out), F32),
            vm((n_l + 1, 4, 1, vec // 2), F32), vm((n_l + 1, 4, 1, rows_out // 2), F32),
            vm((n_l + 1, 2, 1, vec // 2), F32), vm((n_l + 1, 2, 1, rows_out // 2), F32),
            vm((n_m + 2, TP, 1, 2 * LANES), F32), vm((n_m + 2, TP, 1, LANES), F32),
            vm((n_m + 4, 2, 1, LANES), F32), vm((n_m + 2, 4, 1, LANES), F32),
            vm((8, LANES), F32), vm((8, LANES), F32), vm((LANES, LANES), F32),
            sem((2 + n_m,)), sem((3,)), sem((2, 2)), sem((4,)), sem((3,)), sem((2, PARTS)), sem((2 + n_m,)),
            sem((2,)), sem((n_m, 4)), sem((2,)), sem((n_m, 2)),
            sem((2,)), sem((n_m, 2)), sem((n_m, 4)), sem((2, PARTS)), sem((2,)), sem((2,)), sem((10,)), sem((n_m, 7)),
            pltpu.SemaphoreType.REGULAR((2,)),
        ],
        compiler_params=pltpu.CompilerParams(collective_id=0, has_side_effects=True, vmem_limit_bytes=34 * 2 ** 20),
        name='fused_update',
    )(g_in, g_out, w_in, w_out, m_in, m_out, r_in, c_in, r_out, c_out, lr.reshape(1), wd.reshape(1), b2.reshape(1))
    return tuple(pl.pallas_call(
        store_kernel,
        out_shape=tuple(jax.ShapeDtypeStruct(a.shape, a.dtype) for a in outs),
        in_specs=[vmem] * 8,
        out_specs=[hbm] * 8,
        scratch_shapes=[sem((8,))],
        compiler_params=pltpu.CompilerParams(vmem_limit_bytes=2 ** 20),
        name='store_out',
    )(*res))


def solution(mesh):
    in_specs = (P(None, None, 'tp'), P(None, 'tp', None), P('dp', None, None, 'tp'), P('dp', None, 'tp', None), P(None, 'dp', 'tp'), P(None, 'tp', 'dp'), P(None, 'dp'), P(None, 'tp'), P(None, 'tp'), P(None, 'dp'), P(), P(), P())
    out_specs = (P(None, None, 'tp'), P(None, 'tp', None), P(None, 'dp', 'tp'), P(None, 'tp', 'dp'), P(None, 'dp'), P(None, 'tp'), P(None, 'tp'), P(None, 'dp'))
    return jax.shard_map(local_step, mesh=mesh, in_specs=in_specs, out_specs=out_specs, check_vma=False)
```

```python
import jax
import jax.numpy as jnp
from jax import lax
from jax.experimental import pallas as pl
from jax.experimental.pallas import tpu as pltpu
from jax.sharding import PartitionSpec as P

MESH = pl.DeviceIdType.MESH
F32 = jnp.float32
LANES = 128
TP, DP = 4, 8
PARTS = 8
STORES = 8


def total(x):
    return jnp.sum(jnp.sum(x, axis=0, keepdims=True), axis=1, keepdims=True)


def eye_mask():
    row = lax.broadcasted_iota(jnp.int32, (LANES, LANES), 0)
    col = lax.broadcasted_iota(jnp.int32, (LANES, LANES), 1)
    return row == col


def to_row(col):
    return jnp.sum(jnp.where(eye_mask(), jnp.broadcast_to(col, (LANES, LANES)), 0.0), axis=0, keepdims=True)


def to_rows(row):
    col = jnp.sum(jnp.where(eye_mask(), jnp.broadcast_to(row, (LANES, LANES)), 0.0), axis=1, keepdims=True)
    return jnp.broadcast_to(col, (LANES, LANES))


def fused_kernel(g_in, g_out, w_in, w_out, m_in, m_out, r_in, c_in, r_out, c_out, lr_ref, wd_ref, b2_ref,
                 ow_in, ow_out, om_in, om_out, or_in, oc_in, or_out, oc_out,
                 gm_in, gm_out, r1_in, r1_out, r2_in, r2_out, ws_in, ws_out,
                 vr_in, vc_in, vr_out, vc_out, vp_in, vp_out, vh_in, vh_out, vf_in, vf_out, ts, tr, rp, rc, short, olds, rb,
                 ld_sem, pre_sem, d2_send, d2_first, d2_recv, p1_send, p1_recv, p2_send, p2_recv,
                 a_send, a1_recv, a2_recv, a2_last, ad_send, ad_recv, v_send, v_recv, z_sem):
    t = lax.axis_index('tp')
    d = lax.axis_index('dp')
    core = lax.rem(d, 2)
    chip = d // 2
    x = lax.rem(chip, 2)
    y = chip // 2
    k_own = chip
    k_x = y * 2 + (1 - x)
    k_y = (1 - y) * 2 + x
    k_d = (1 - y) * 2 + (1 - x)
    dev_x = k_x * 2 + core
    dev_y = k_y * 2 + core
    dev_d = k_d * 2 + core
    dev_c = chip * 2 + (1 - core)
    lr = lr_ref[0]
    wd = wd_ref[0]
    b2 = b2_ref[0]
    n_layers = gm_in.shape[0]
    mats = [(0, i) for i in range(n_layers)] + [(1, i) for i in range(n_layers)]
    n_mats = len(mats)
    sw = gm_in.shape[2]
    half_in = sw // 2
    cols_in = gm_in.shape[3]
    rows_out = gm_out.shape[2]
    half_out = rows_out // 2

    def full_view(refs, mat, q, h, lead):
        kind, l = mat
        pre = (0,) if lead else ()
        if kind == 0:
            return refs[0].at[pre + (l, pl.ds(pl.multiple_of(q * sw + h * half_in, half_in), half_in), slice(None))]
        return refs[1].at[pre + (l, pl.ds(h * half_out, half_out), pl.ds(pl.multiple_of(q * LANES, LANES), LANES))]

    def full_shard(refs, mat, q):
        kind, l = mat
        if kind == 0:
            return refs[0].at[l, pl.ds(pl.multiple_of(q * sw, sw), sw), :]
        return refs[1].at[l, :, pl.ds(pl.multiple_of(q * LANES, LANES), LANES)]

    def half_view(refs, mat, k, h):
        kind, l = mat
        size = half_in if kind == 0 else half_out
        return refs[kind].at[l, k, pl.ds(h * size, size)]

    gs = (g_in, g_out)
    ows = (ow_in, ow_out)
    gms = (gm_in, gm_out)
    r1s = (r1_in, r1_out)
    r2s = (r2_in, r2_out)
    oms = (om_in, om_out)
    wss = (ws_in, ws_out)

    def remote(src, dst, send, recv, dev_t, dev_d):
        cp = pltpu.make_async_remote_copy(src_ref=src, dst_ref=dst, send_sem=send, recv_sem=recv,
                                          device_id=(dev_t, dev_d), device_id_type=MESH)
        cp.start()
        return cp

    def wait_bytes(ref, sem):
        pltpu.make_async_copy(ref, ref, sem).wait()

    def add_into(dst, src):
        rows, cols = dst.shape
        step = 8 if cols > LANES else 128
        if rows % step:
            step = 8

        def body(i, carry):
            sl = pl.ds(pl.multiple_of(i * step, step), step)
            dst[sl, :] = dst[sl, :] + src[sl, :]
            return carry

        lax.fori_loop(0, rows // step, body, 0)

    pieces = [(k_d, 0), (k_d, 1), (k_x, 0), (k_y, 1), (k_y, 0), (k_x, 1), (k_own, 0), (k_own, 1)]
    routes = [(0, 1, dev_x), (1, 1, dev_y), (0, 0, dev_x), (1, 0, dev_y)]

    def sub(ref, i):
        rows = ref.shape[0] // PARTS
        return ref.at[pl.ds(i * rows, rows)]

    def start_loads(m):
        mat = mats[m]
        for k, h in pieces:
            pltpu.make_async_copy(full_view(gs, mat, 2 * k + core, h, True), half_view(gms, mat, k, h), ld_sem.at[2 + m]).start()

    def load_first(lo, hi):
        for i in range(lo, hi):
            k, h = pieces[i]
            q = 2 * k + (1 - core)
            pltpu.make_async_copy(full_view(gs, mats[0], q, h, True), full_view(ows, mats[0], q, h, False), pre_sem.at[min(i, 2)]).start()
            pltpu.make_async_copy(full_view(gs, mats[0], 2 * k + core, h, True), half_view(gms, mats[0], k, h), ld_sem.at[min(i, 2)]).start()

    def swap_first():
        views = [full_view(ows, mats[0], 2 * k + (1 - core), h, False) for k, h in pieces]
        for i in range(2):
            wait_bytes(views[i], pre_sem.at[i])
            remote(sub(views[i], 0), sub(views[i], 0), d2_send.at[2], d2_first.at[0], t, dev_c)
        for p in range(1, PARTS):
            for i in range(2):
                remote(sub(views[i], p), sub(views[i], p), d2_send.at[2], d2_first.at[p], t, dev_c)

    def swap_rest():
        views = [full_view(ows, mats[0], 2 * k + (1 - core), h, False) for k, h in pieces]
        wait_bytes(gm_in.at[0, pl.ds(0, 3)], pre_sem.at[2])
        for i in range(2, 8):
            remote(views[i], views[i], d2_send.at[2], d2_recv.at[min(i - 2, 2)], t, dev_c)

    def start_swap(m):
        mat = mats[m]
        for k, h in pieces:
            q = 2 * k + (1 - core)
            remote(full_view(gs, mat, q, h, True), full_view(ows, mat, q, h, False), d2_send.at[mat[0]], d2_recv.at[2 + m], t, dev_c)

    def chip_views(m, i):
        k, h = pieces[i]
        return half_view(gms, mats[m], k, h), full_view(ows, mats[m], 2 * k + core, h, False)

    def send_first(m, i, part=None):
        kind, l = mats[m]
        h, j, dev = routes[i]
        mine, other = chip_views(m, i)
        dst = r1s[kind].at[l, h, j]
        if part is not None:
            mine, other, dst = sub(mine, part), sub(other, part), sub(dst, part)
        add_into(mine, other)
        remote(mine, dst, p1_send.at[kind], p1_recv.at[m, j], t, dev)

    def stage_a_first():
        views = [chip_views(0, i)[0] for i in range(8)]
        for i in range(2):
            wait_bytes(views[i], ld_sem.at[i])
        for p in range(PARTS):
            wait_bytes(sub(gm_in.at[0, 0], p), d2_first.at[p])
            for i in range(2):
                send_first(0, i, p)
        swap_rest()
        wait_bytes(gm_in.at[0, pl.ds(0, 3)], ld_sem.at[2])
        for i in range(2, 4):
            wait_bytes(views[i], d2_recv.at[i - 2])
            send_first(0, i)

    def keep_first(m):
        for i in range(4, 8):
            add_into(*chip_views(m, i))

    def stage_a(m):
        kind, l = mats[m]
        gm = gms[kind].at[l]
        wait_bytes(gm, ld_sem.at[2 + m])
        wait_bytes(gm, d2_recv.at[2 + m])
        for i in range(4):
            send_first(m, i)
        keep_first(m)

    def stage_b(m):
        kind, l = mats[m]
        pair = gms[kind].at[l, 0]
        wait_bytes(pair, p1_recv.at[m, 1])
        for h, k, dev in ((0, k_y, dev_y), (1, k_x, dev_x)):
            mine = half_view(gms, mats[m], k, h)
            add_into(mine, r1s[kind].at[l, h, 1])
            remote(mine, r2s[kind].at[l, h], p2_send.at[kind], p2_recv.at[m], t, dev)
        wait_bytes(pair, p1_recv.at[m, 0])
        for h in range(2):
            add_into(half_view(gms, mats[m], k_own, h), r1s[kind].at[l, h, 0])

    vps = (vp_in, vp_out)
    vhs = (vh_in, vh_out)
    vfs = (vf_in, vf_out)

    def send_chips(slots, send, recv):
        for dev in (dev_x, dev_y, dev_d):
            remote(slots.at[chip], slots.at[chip], send, recv, t, dev)

    def send_core(slots, send, recv):
        remote(slots.at[core], slots.at[core], send, recv, t, dev_c)

    def send_tp(slots, send, recv):
        for i in range(1, TP):
            remote(slots.at[t], slots.at[t], send, recv, lax.rem(t + i, TP), d)

    def sum_slots(slots, count):
        acc = slots[0]
        for i in range(1, count):
            acc = acc + slots[i]
        return acc

    def stage_c(m):
        kind, l = mats[m]
        mat = mats[m]
        wait_bytes(gms[kind].at[l, 0], p2_recv.at[m])
        for h in range(2):
            add_into(half_view(gms, mat, k_own, h), r2s[kind].at[l, h])
        own = vps[kind].at[l, core]
        shard = gms[kind].at[l, k_own]
        if kind == 0:
            def body(i, acc):
                sl = pl.ds(pl.multiple_of(i * 8, 8), 8)
                g = shard[sl, :]
                s = g * g + 1e-30
                rb[sl, :] = jnp.broadcast_to(jnp.sum(s, axis=1, keepdims=True), (8, LANES))
                return acc + s

            acc = lax.fori_loop(0, sw // 8, body, jnp.zeros((8, cols_in), F32))
            own[:, pl.ds(0, cols_in)] = jnp.sum(acc, axis=0, keepdims=True)
            own[:, pl.ds(cols_in, LANES)] = vr_in[pl.ds(l, 1), :]
            spare = own.shape[1] - cols_in - LANES
            if spare:
                own[:, pl.ds(cols_in + LANES, spare)] = jnp.zeros((1, spare), F32)
            short[pl.ds(m, 1), :] = to_row(rb[pl.ds(0, LANES), 0:1])
        else:
            def body(i, acc):
                g = shard[pl.ds(pl.multiple_of(i * LANES, LANES), LANES), :]
                s = g * g + 1e-30
                own[:, pl.ds(pl.multiple_of(i * LANES, LANES), LANES)] = to_row(jnp.sum(s, axis=1, keepdims=True))
                return acc + jnp.sum(s, axis=0, keepdims=True)

            short[pl.ds(m, 1), :] = lax.fori_loop(0, rows_out // LANES, body, jnp.zeros((1, LANES), F32))
        send_core(vps[kind].at[l], v_send.at[0], v_recv.at[m, 0])

    def stage_k(m):
        kind, l = mats[m]
        both = vps[kind].at[l]
        wait_bytes(both.at[0], v_recv.at[m, 0])
        size = vhs[kind].shape[3]
        half = pl.ds(pl.multiple_of(core * size, LANES), size)
        vhs[kind].at[l, chip][...] = both.at[0][:, half] + both.at[1][:, half]
        send_chips(vhs[kind].at[l], v_send.at[0], v_recv.at[m, 1])

    def stage_d(m):
        kind, l = mats[m]
        slots = vhs[kind].at[l]
        wait_bytes(slots.at[pl.ds(0, 3)], v_recv.at[m, 1])
        vfs[kind].at[l, core][...] = sum_slots(slots, 4)
        send_core(vfs[kind].at[l], v_send.at[0], v_recv.at[m, 2])

    in_rows, in_cols = sw * DP, cols_in * TP
    out_rows, out_cols = rows_out * TP, sw * DP

    def stage_l(m):
        kind, l = mats[m]
        both = vfs[kind].at[l]
        wait_bytes(both.at[0], v_recv.at[m, 2])
        acc = jnp.concatenate([both[0], both[1]], axis=1)
        own = ts.at[m, t]
        own[:, pl.ds(0, LANES)] = short[pl.ds(m, 1), :]
        if kind == 0:
            col_sum = acc[:, :cols_in]
            oc_in[pl.ds(l, 1), :] = b2 * vc_in[pl.ds(l, 1), :] + (1.0 - b2) * (col_sum / in_rows)
            plane = jnp.sum(col_sum, axis=1, keepdims=True)
            olds[pl.ds(l, 1), :] = acc[:, cols_in:cols_in + LANES]
        else:
            r_new = b2 * vr_out[pl.ds(l, 1), :] + (1.0 - b2) * (acc / out_cols)
            or_out[pl.ds(l, 1), :] = r_new
            plane = jnp.sum(r_new, axis=1, keepdims=True)
        own[:, pl.ds(LANES, LANES)] = jnp.broadcast_to(plane, (1, LANES))
        send_tp(ts.at[m], v_send.at[0], v_recv.at[m, 3])

    def stage_e(m):
        kind, l = mats[m]
        wait_bytes(ts.at[m, pl.ds(0, TP - 1)], v_recv.at[m, 3])
        acc = sum_slots(ts.at[m], TP)
        vec = acc[:, :LANES]
        tot = acc[:, LANES:LANES + 1]
        shard = gms[kind].at[l, k_own]
        if kind == 0:
            r_new = b2 * vr_in[pl.ds(l, 1), :] + (1.0 - b2) * (vec / in_cols)
            or_in[pl.ds(l, 1), :] = r_new
            old = jnp.sum(olds[pl.ds(l, 1), :], axis=1, keepdims=True)
            avg = (b2 * old + (1.0 - b2) * (tot / in_cols)) / in_rows
            rb[pl.ds(0, LANES), :] = to_rows(1.0 / jnp.sqrt(r_new))
            cj = jnp.sqrt(avg) / jnp.sqrt(oc_in[pl.ds(l, 1), :])

            def body(i, acc):
                sl = pl.ds(pl.multiple_of(i * 8, 8), 8)
                u = (shard[sl, :] * rb[sl, 0:1]) * cj
                shard[sl, :] = u
                return acc + u * u

            sq = lax.fori_loop(0, sw // 8, body, jnp.zeros((8, cols_in), F32))
        else:
            c_new = b2 * vc_out[pl.ds(l, 1), :] + (1.0 - b2) * (vec / out_rows)
            oc_out[pl.ds(l, 1), :] = c_new
            avg = tot / out_rows
            cj = jnp.sqrt(avg) / jnp.sqrt(c_new)

            def body(i, acc):
                sl = pl.ds(pl.multiple_of(i * LANES, LANES), LANES)
                ri = to_rows(1.0 / jnp.sqrt(or_out[pl.ds(l, 1), sl]))
                u = (shard[sl, :] * ri) * cj
                shard[sl, :] = u
                return acc + u * u

            sq = lax.fori_loop(0, rows_out // LANES, body, jnp.zeros((LANES, LANES), F32))
        tr.at[m, t][...] = jnp.broadcast_to(total(sq), (1, LANES))
        send_tp(tr.at[m], v_send.at[0], v_recv.at[m, 4])

    def stage_f(m):
        wait_bytes(tr.at[m, pl.ds(0, TP - 1)], v_recv.at[m, 4])
        rp.at[m, core][...] = sum_slots(tr.at[m], TP)
        send_core(rp.at[m], v_send.at[0], v_recv.at[m, 0])

    def stage_n(m):
        wait_bytes(rp.at[m, 0], v_recv.at[m, 0])
        rc.at[m, chip][...] = rp.at[m][0] + rp.at[m][1]
        send_chips(rc.at[m], v_send.at[0], v_recv.at[m, 5])

    def stage_g(m):
        mat = mats[m]
        kind, l = mat
        wait_bytes(rc.at[m, pl.ds(0, 3)], v_recv.at[m, 5])
        size = float(in_rows * in_cols if kind == 0 else out_rows * out_cols)
        rms = jnp.sqrt(sum_slots(rc.at[m], 4) / size)
        scale = (1.0 / jnp.maximum(1.0, rms))[:, 0:1]
        shard = gms[kind].at[l, k_own]
        mom = oms[kind].at[l]
        old = wss[kind].at[l]
        new = full_shard(ows, mat, d)
        if l == 0:
            wait_bytes(oms[kind], pre_sem.at[2 * kind])
            wait_bytes(wss[kind], pre_sem.at[2 * kind + 1])
        step = 16 if kind == 0 else 128

        def body(i, carry):
            sl = pl.ds(pl.multiple_of(i * step, step), step)
            mn = (0.9 * mom[sl, :].astype(F32) + 0.1 * (shard[sl, :] * scale)).astype(jnp.bfloat16)
            mom[sl, :] = mn
            w = old[sl, :]
            new[sl, :] = w - lr * mn.astype(F32) - lr * wd * w
            return carry

        lax.fori_loop(0, shard.shape[0] // step, body, 0)
        q = d
        a = full_view(ows, mat, q, 0, False)
        b = full_view(ows, mat, q, 1, False)
        remote(a, a, a_send.at[kind], a1_recv.at[m], t, dev_y)
        remote(b, b, a_send.at[kind], a1_recv.at[m], t, dev_x)
        remote(a, a, a_send.at[kind], a2_recv.at[m, 0], t, dev_x)
        remote(b, b, a_send.at[kind], a2_recv.at[m, 0], t, dev_y)
        pass_core(m, new)

    def pass_core(m, view):
        kind = mats[m][0]
        remote(view, view, ad_send.at[kind], ad_recv.at[kind], t, dev_c)

    def stage_h(m):
        mat = mats[m]
        kind = mat[0]
        a = full_view(ows, mat, 2 * k_y + core, 0, False)
        b = full_view(ows, mat, 2 * k_x + core, 1, False)
        wait_bytes(gms[kind].at[mat[1], 0], a1_recv.at[m])
        for view, dev in ((a, dev_x), (b, dev_y)):
            if m < n_mats - 1:
                remote(view, view, a_send.at[kind], a2_recv.at[m, 1], t, dev)
            else:
                for p in range(PARTS):
                    remote(sub(view, p), sub(view, p), a_send.at[kind], a2_last.at[p], t, dev)
        pass_core(m, a)
        pass_core(m, b)

    def stage_i(m):
        kind, l = mats[m]
        pair = gms[kind].at[l, 0]
        wait_bytes(pair, a2_recv.at[m, 0])
        pass_core(m, full_view(ows, mats[m], 2 * k_x + core, 0, False))
        pass_core(m, full_view(ows, mats[m], 2 * k_y + core, 1, False))
        views = [full_view(ows, mats[m], 2 * k_d + core, h, False) for h in range(2)]
        if m < n_mats - 1:
            wait_bytes(pair, a2_recv.at[m, 1])
            for view in views:
                pass_core(m, view)
        else:
            for p in range(PARTS):
                wait_bytes(sub(pair, p), a2_last.at[p])
                for view in views:
                    pass_core(m, sub(view, p))

    small = [(r_in, vr_in), (c_in, vc_in), (r_out, vr_out), (c_out, vc_out)]
    barrier = pltpu.get_barrier_semaphore()
    z_low = jnp.minimum(t, 1)
    z_high = jnp.minimum(TP - 1 - t, 1)

    def signal_low(sem):
        @pl.when(t > 0)
        def _():
            pl.semaphore_signal(sem, inc=1, device_id=(t - 1, d), device_id_type=MESH)

    def signal_high(sem):
        @pl.when(t < TP - 1)
        def _():
            pl.semaphore_signal(sem, inc=1, device_id=(t + 1, d), device_id_type=MESH)

    for dev in (dev_x, dev_y, dev_c):
        pl.semaphore_signal(barrier, inc=1, device_id=(t, dev), device_id_type=MESH)
    signal_high(barrier)
    load_first(0, 2)
    load_first(2, 8)
    pl.semaphore_wait(barrier, 3 + z_low)
    swap_first()
    stage_a_first()
    start_loads(1)
    start_swap(1)
    signal_low(z_sem.at[0])
    wait_bytes(gm_in.at[0, pl.ds(0, 2)], d2_recv.at[2])
    keep_first(0)
    stage_a(1)
    for i, (src, dst) in enumerate(small):
        pltpu.make_async_copy(src, dst, ld_sem.at[i]).start()
    for m, (kind, l) in enumerate(mats):
        pltpu.make_async_copy((m_in, m_out)[kind].at[l], oms[kind].at[l], pre_sem.at[2 * kind]).start()
        src = w_in.at[l, pl.ds(pl.multiple_of(d * sw, sw), sw), :] if kind == 0 else w_out.at[l, :, pl.ds(pl.multiple_of(d * LANES, LANES), LANES)]
        pltpu.make_async_copy(src, wss[kind].at[l], pre_sem.at[2 * kind + 1]).start()
    wait_bytes(gm_in.at[0], d2_send.at[2])

    @pl.when(t < TP - 1)
    def _():
        pl.semaphore_wait(z_sem.at[0], 1)

    signal_low(z_sem.at[1])
    signal_high(z_sem.at[1])
    for i, (src, dst) in enumerate(small):
        wait_bytes(dst, ld_sem.at[i])
    order = 's2 b0 a2 s3 b1 c0 k0 a3 b2 c1 k1 d0 l0 e0 f0 n0 b3 c2 k2 g0 d1 l1 e1 f1 n1 c3 k3 d2 l2 h0 e2 f2 n2 g1 i0 d3 l3 e3 f3 n3 h1 g2 i1 h2 g3 i2 h3 i3'
    def stage_s(m):
        start_loads(m)
        start_swap(m)

    stages = dict(s=stage_s, a=stage_a, b=stage_b, c=stage_c, d=stage_d, e=stage_e, f=stage_f, g=stage_g, h=stage_h, i=stage_i, k=stage_k, l=stage_l, n=stage_n)
    pl.semaphore_wait(z_sem.at[1], z_low + z_high)
    signal_low(z_sem.at[2])
    signal_high(z_sem.at[2])
    pl.semaphore_wait(z_sem.at[2], z_low + z_high)
    for item in order.split():
        stages[item[0]](int(item[1]))
    for kind in range(2):
        gm = gms[kind]
        wait_bytes(gm, ad_recv.at[kind])
        wait_bytes(gm.at[pl.ds(0, n_layers - 1 + kind)], d2_send.at[kind])
        wait_bytes(r1s[kind], p1_send.at[kind])
        wait_bytes(r2s[kind], p2_send.at[kind])
        wait_bytes(gm.at[:, pl.ds(0, 3)], a_send.at[kind])
        wait_bytes(gm, ad_send.at[kind])
    sizes = [n_layers * (vps[k].shape[3] + (3 + 1) * vhs[k].shape[3]) for k in range(2)]
    sent = sum(sizes) + n_mats * ((TP - 1) * 3 + 1 + 3) * LANES
    wait_bytes(gm_out.at[0, 0, pl.ds(0, sent // LANES)], v_send.at[0])


def store_kernel(*refs):
    n = (len(refs) - 1) // 2
    sems = refs[-1]
    for i in range(n):
        src, dst = refs[i], refs[n + i]
        if i < 2:
            rows = src.shape[1] // STORES
            for l in range(src.shape[0]):
                for c in range(STORES):
                    pltpu.make_async_copy(src.at[l, pl.ds(c * rows, rows)], dst.at[l, pl.ds(c * rows, rows)], sems.at[i]).start()
        else:
            pltpu.make_async_copy(src, dst, sems.at[i]).start()
    for i in range(n):
        pltpu.make_async_copy(refs[i], refs[n + i], sems.at[i]).wait()


def local_step(w_in, w_out, g_in, g_out, m_in, m_out, r_in, c_in, r_out, c_out, lr, wd, b2):
    n_l, rows_in, cols_in = w_in.shape
    rows_out = w_out.shape[1]
    sw = rows_in // DP
    n_m = 2 * n_l
    vec = (cols_in + LANES + 2 * LANES - 1) // (2 * LANES) * (2 * LANES)
    hbm = pl.BlockSpec(memory_space=pltpu.HBM)
    vmem = pl.BlockSpec(memory_space=pltpu.VMEM)
    smem = pl.BlockSpec(memory_space=pltpu.SMEM)
    vm = pltpu.VMEM
    sem = pltpu.SemaphoreType.DMA
    outs = (w_in, w_out, m_in, m_out, r_in, c_in, r_out, c_out)
    res = pl.pallas_call(
        fused_kernel,
        out_shape=tuple(vm(a.shape, a.dtype) for a in outs),
        in_specs=[hbm] * 10 + [smem] * 3,
        out_specs=[vmem] * 8,
        scratch_shapes=[
            vm((n_l, 4, sw, cols_in), F32), vm((n_l, 4, rows_out, LANES), F32),
            vm((n_l, 2, 2, sw // 2, cols_in), F32), vm((n_l, 2, 2, rows_out // 2, LANES), F32),
            vm((n_l, 2, sw // 2, cols_in), F32), vm((n_l, 2, rows_out // 2, LANES), F32),
            vm((n_l, sw, cols_in), F32), vm((n_l, rows_out, LANES), F32),
            vm(r_in.shape, F32), vm(c_in.shape, F32), vm(r_out.shape, F32), vm(c_out.shape, F32),
            vm((n_l + 1, 2, 1, vec), F32), vm((n_l + 1, 2, 1, rows_out), F32),
            vm((n_l + 1, 4, 1, vec // 2), F32), vm((n_l + 1, 4, 1, rows_out // 2), F32),
            vm((n_l + 1, 2, 1, vec // 2), F32), vm((n_l + 1, 2, 1, rows_out // 2), F32),
            vm((n_m + 2, TP, 1, 2 * LANES), F32), vm((n_m + 2, TP, 1, LANES), F32),
            vm((n_m + 4, 2, 1, LANES), F32), vm((n_m + 2, 4, 1, LANES), F32),
            vm((8, LANES), F32), vm((8, LANES), F32), vm((LANES, LANES), F32),
            sem((2 + n_m,)), sem((4,)), sem((3,)), sem((PARTS,)), sem((2 + n_m,)),
            sem((2,)), sem((n_m, 2)), sem((2,)), sem((n_m,)),
            sem((2,)), sem((n_m,)), sem((n_m, 2)), sem((PARTS,)), sem((2,)), sem((2,)), sem((1,)), sem((n_m, 6)),
            pltpu.SemaphoreType.REGULAR((3,)),
        ],
        compiler_params=pltpu.CompilerParams(collective_id=0, has_side_effects=True, vmem_limit_bytes=34 * 2 ** 20),
        name='fused_update',
    )(g_in, g_out, w_in, w_out, m_in, m_out, r_in, c_in, r_out, c_out, lr.reshape(1), wd.reshape(1), b2.reshape(1))
    return tuple(pl.pallas_call(
        store_kernel,
        out_shape=tuple(jax.ShapeDtypeStruct(a.shape, a.dtype) for a in outs),
        in_specs=[vmem] * 8,
        out_specs=[hbm] * 8,
        scratch_shapes=[sem((8,))],
        compiler_params=pltpu.CompilerParams(vmem_limit_bytes=2 ** 20),
        name='store_out',
    )(*res))


def solution(mesh):
    in_specs = (P(None, None, 'tp'), P(None, 'tp', None), P('dp', None, None, 'tp'), P('dp', None, 'tp', None), P(None, 'dp', 'tp'), P(None, 'tp', 'dp'), P(None, 'dp'), P(None, 'tp'), P(None, 'tp'), P(None, 'dp'), P(), P(), P())
    out_specs = (P(None, None, 'tp'), P(None, 'tp', None), P(None, 'dp', 'tp'), P(None, 'tp', 'dp'), P(None, 'dp'), P(None, 'tp'), P(None, 'tp'), P(None, 'dp'))
    return jax.shard_map(local_step, mesh=mesh, in_specs=in_specs, out_specs=out_specs, check_vma=False)
```

```python
import jax
import jax.numpy as jnp
from jax import lax
from jax.experimental import pallas as pl
from jax.experimental.pallas import tpu as pltpu
from jax.sharding import PartitionSpec as P

MESH = pl.DeviceIdType.MESH
F32 = jnp.float32
LANES = 128
TP, DP = 4, 8
PARTS = 8
STORES = 8


def total(x):
    return jnp.sum(jnp.sum(x, axis=0, keepdims=True), axis=1, keepdims=True)


def eye_mask():
    row = lax.broadcasted_iota(jnp.int32, (LANES, LANES), 0)
    col = lax.broadcasted_iota(jnp.int32, (LANES, LANES), 1)
    return row == col


def to_row(col):
    return jnp.sum(jnp.where(eye_mask(), jnp.broadcast_to(col, (LANES, LANES)), 0.0), axis=0, keepdims=True)


def to_rows(row):
    col = jnp.sum(jnp.where(eye_mask(), jnp.broadcast_to(row, (LANES, LANES)), 0.0), axis=1, keepdims=True)
    return jnp.broadcast_to(col, (LANES, LANES))


def fused_kernel(g_in, g_out, w_in, w_out, m_in, m_out, r_in, c_in, r_out, c_out, lr_ref, wd_ref, b2_ref,
                 ow_in, ow_out, om_in, om_out, or_in, oc_in, or_out, oc_out,
                 gm_in, gm_out, r1_in, r1_out, r2_in, r2_out, ws_in, ws_out,
                 vr_in, vc_in, vr_out, vc_out, vp_in, vp_out, vh_in, vh_out, vf_in, vf_out, ts, tr, rp, rc, short, olds, rb,
                 ld_sem, pre_sem, d2_send, d2_first, d2_recv, p1_send, p1_recv, p2_send, p2_recv,
                 a_send, a2_last, ad_send, v_send, v_recv, z_sem):
    t = lax.axis_index('tp')
    d = lax.axis_index('dp')
    core = lax.rem(d, 2)
    chip = d // 2
    x = lax.rem(chip, 2)
    y = chip // 2
    k_own = chip
    k_x = y * 2 + (1 - x)
    k_y = (1 - y) * 2 + x
    k_d = (1 - y) * 2 + (1 - x)
    dev_x = k_x * 2 + core
    dev_y = k_y * 2 + core
    dev_d = k_d * 2 + core
    dev_c = chip * 2 + (1 - core)
    lr = lr_ref[0]
    wd = wd_ref[0]
    b2 = b2_ref[0]
    n_layers = gm_in.shape[0]
    mats = [(0, i) for i in range(n_layers)] + [(1, i) for i in range(n_layers)]
    n_mats = len(mats)
    sw = gm_in.shape[2]
    half_in = sw // 2
    cols_in = gm_in.shape[3]
    rows_out = gm_out.shape[2]
    half_out = rows_out // 2

    def full_view(refs, mat, q, h, lead):
        kind, l = mat
        pre = (0,) if lead else ()
        if kind == 0:
            return refs[0].at[pre + (l, pl.ds(pl.multiple_of(q * sw + h * half_in, half_in), half_in), slice(None))]
        return refs[1].at[pre + (l, pl.ds(h * half_out, half_out), pl.ds(pl.multiple_of(q * LANES, LANES), LANES))]

    def full_shard(refs, mat, q):
        kind, l = mat
        if kind == 0:
            return refs[0].at[l, pl.ds(pl.multiple_of(q * sw, sw), sw), :]
        return refs[1].at[l, :, pl.ds(pl.multiple_of(q * LANES, LANES), LANES)]

    def half_view(refs, mat, k, h):
        kind, l = mat
        size = half_in if kind == 0 else half_out
        return refs[kind].at[l, k, pl.ds(h * size, size)]

    gs = (g_in, g_out)
    ows = (ow_in, ow_out)
    gms = (gm_in, gm_out)
    r1s = (r1_in, r1_out)
    r2s = (r2_in, r2_out)
    oms = (om_in, om_out)
    wss = (ws_in, ws_out)

    def remote(src, dst, send, recv, dev_t, dev_d):
        cp = pltpu.make_async_remote_copy(src_ref=src, dst_ref=dst, send_sem=send, recv_sem=recv,
                                          device_id=(dev_t, dev_d), device_id_type=MESH)
        cp.start()
        return cp

    def wait_bytes(ref, sem):
        pltpu.make_async_copy(ref, ref, sem).wait()

    def add_into(dst, src):
        rows, cols = dst.shape
        step = 8 if cols > LANES else 128
        if rows % step:
            step = 8

        def body(i, carry):
            sl = pl.ds(pl.multiple_of(i * step, step), step)
            dst[sl, :] = dst[sl, :] + src[sl, :]
            return carry

        lax.fori_loop(0, rows // step, body, 0)

    pieces = [(k_d, 0), (k_d, 1), (k_x, 0), (k_y, 1), (k_y, 0), (k_x, 1), (k_own, 0), (k_own, 1)]
    routes = [(0, 1, dev_x), (1, 1, dev_y), (0, 0, dev_x), (1, 0, dev_y)]

    def sub(ref, i):
        rows = ref.shape[0] // PARTS
        return ref.at[pl.ds(i * rows, rows)]

    def start_loads(m):
        mat = mats[m]
        for k, h in pieces:
            pltpu.make_async_copy(full_view(gs, mat, 2 * k + core, h, True), half_view(gms, mat, k, h), ld_sem.at[2 + m]).start()

    def load_first(lo, hi):
        for i in range(lo, hi):
            k, h = pieces[i]
            q = 2 * k + (1 - core)
            pltpu.make_async_copy(full_view(gs, mats[0], q, h, True), full_view(ows, mats[0], q, h, False), pre_sem.at[min(i, 2)]).start()
            pltpu.make_async_copy(full_view(gs, mats[0], 2 * k + core, h, True), half_view(gms, mats[0], k, h), ld_sem.at[min(i, 2)]).start()

    def swap_first():
        views = [full_view(ows, mats[0], 2 * k + (1 - core), h, False) for k, h in pieces]
        for i in range(2):
            wait_bytes(views[i], pre_sem.at[i])
            remote(sub(views[i], 0), sub(views[i], 0), d2_send.at[2], d2_first.at[0], t, dev_c)
        for p in range(1, PARTS):
            for i in range(2):
                remote(sub(views[i], p), sub(views[i], p), d2_send.at[2], d2_first.at[p], t, dev_c)

    def swap_rest():
        views = [full_view(ows, mats[0], 2 * k + (1 - core), h, False) for k, h in pieces]
        wait_bytes(gm_in.at[0, pl.ds(0, 3)], pre_sem.at[2])
        for i in range(2, 8):
            remote(views[i], views[i], d2_send.at[2], d2_recv.at[min(i - 2, 2)], t, dev_c)

    def start_swap(m):
        mat = mats[m]
        for k, h in pieces:
            q = 2 * k + (1 - core)
            remote(full_view(gs, mat, q, h, True), full_view(ows, mat, q, h, False), d2_send.at[mat[0]], d2_recv.at[2 + m], t, dev_c)

    def chip_views(m, i):
        k, h = pieces[i]
        return half_view(gms, mats[m], k, h), full_view(ows, mats[m], 2 * k + core, h, False)

    def send_first(m, i, part=None):
        kind, l = mats[m]
        h, j, dev = routes[i]
        mine, other = chip_views(m, i)
        dst = r1s[kind].at[l, h, j]
        if part is not None:
            mine, other, dst = sub(mine, part), sub(other, part), sub(dst, part)
        add_into(mine, other)
        remote(mine, dst, p1_send.at[kind], p1_recv.at[m, j], t, dev)

    def stage_a_first():
        views = [chip_views(0, i)[0] for i in range(8)]
        for i in range(2):
            wait_bytes(views[i], ld_sem.at[i])
        for p in range(PARTS):
            wait_bytes(sub(gm_in.at[0, 0], p), d2_first.at[p])
            for i in range(2):
                send_first(0, i, p)
        swap_rest()
        wait_bytes(gm_in.at[0, pl.ds(0, 3)], ld_sem.at[2])
        for i in range(2, 4):
            wait_bytes(views[i], d2_recv.at[i - 2])
            send_first(0, i)

    def keep_first(m):
        for i in range(4, 8):
            add_into(*chip_views(m, i))

    def stage_a(m):
        kind, l = mats[m]
        gm = gms[kind].at[l]
        wait_bytes(gm, ld_sem.at[2 + m])
        wait_bytes(gm, d2_recv.at[2 + m])
        for i in range(4):
            send_first(m, i)
        keep_first(m)

    def stage_b(m):
        kind, l = mats[m]
        pair = gms[kind].at[l, 0]
        wait_bytes(pair, p1_recv.at[m, 1])
        for h, k, dev in ((0, k_y, dev_y), (1, k_x, dev_x)):
            mine = half_view(gms, mats[m], k, h)
            add_into(mine, r1s[kind].at[l, h, 1])
            remote(mine, r2s[kind].at[l, h], p2_send.at[kind], p2_recv.at[m], t, dev)
        wait_bytes(pair, p1_recv.at[m, 0])
        for h in range(2):
            add_into(half_view(gms, mats[m], k_own, h), r1s[kind].at[l, h, 0])

    vps = (vp_in, vp_out)
    vhs = (vh_in, vh_out)
    vfs = (vf_in, vf_out)

    def send_chips(slots, send, recv):
        for dev in (dev_x, dev_y, dev_d):
            remote(slots.at[chip], slots.at[chip], send, recv, t, dev)

    def send_core(slots, send, recv):
        remote(slots.at[core], slots.at[core], send, recv, t, dev_c)

    def send_tp(slots, send, recv):
        for i in range(1, TP):
            remote(slots.at[t], slots.at[t], send, recv, lax.rem(t + i, TP), d)

    def sum_slots(slots, count):
        acc = slots[0]
        for i in range(1, count):
            acc = acc + slots[i]
        return acc

    def stage_c(m):
        kind, l = mats[m]
        mat = mats[m]
        wait_bytes(gms[kind].at[l, 0], p2_recv.at[m])
        for h in range(2):
            add_into(half_view(gms, mat, k_own, h), r2s[kind].at[l, h])
        own = vps[kind].at[l, core]
        shard = gms[kind].at[l, k_own]
        if kind == 0:
            def body(i, acc):
                sl = pl.ds(pl.multiple_of(i * 8, 8), 8)
                g = shard[sl, :]
                s = g * g + 1e-30
                rb[sl, :] = jnp.broadcast_to(jnp.sum(s, axis=1, keepdims=True), (8, LANES))
                return acc + s

            acc = lax.fori_loop(0, sw // 8, body, jnp.zeros((8, cols_in), F32))
            own[:, pl.ds(0, cols_in)] = jnp.sum(acc, axis=0, keepdims=True)
            own[:, pl.ds(cols_in, LANES)] = vr_in[pl.ds(l, 1), :]
            spare = own.shape[1] - cols_in - LANES
            if spare:
                own[:, pl.ds(cols_in + LANES, spare)] = jnp.zeros((1, spare), F32)
            short[pl.ds(m, 1), :] = to_row(rb[pl.ds(0, LANES), 0:1])
        else:
            def body(i, acc):
                g = shard[pl.ds(pl.multiple_of(i * LANES, LANES), LANES), :]
                s = g * g + 1e-30
                own[:, pl.ds(pl.multiple_of(i * LANES, LANES), LANES)] = to_row(jnp.sum(s, axis=1, keepdims=True))
                return acc + jnp.sum(s, axis=0, keepdims=True)

            short[pl.ds(m, 1), :] = lax.fori_loop(0, rows_out // LANES, body, jnp.zeros((1, LANES), F32))
        send_core(vps[kind].at[l], v_send.at[0], v_recv.at[3 + m])

    def stage_k(m):
        kind, l = mats[m]
        both = vps[kind].at[l]
        wait_bytes(both.at[0], v_recv.at[3 + m])
        size = vhs[kind].shape[3]
        half = pl.ds(pl.multiple_of(core * size, LANES), size)
        vhs[kind].at[l, chip][...] = both.at[0][:, half] + both.at[1][:, half]
        send_chips(vhs[kind].at[l], v_send.at[0], v_recv.at[3 + n_mats + m])

    def stage_d(m):
        kind, l = mats[m]
        slots = vhs[kind].at[l]
        wait_bytes(slots.at[pl.ds(0, 3)], v_recv.at[3 + n_mats + m])
        vfs[kind].at[l, core][...] = sum_slots(slots, 4)
        send_core(vfs[kind].at[l], v_send.at[0], v_recv.at[0])

    in_rows, in_cols = sw * DP, cols_in * TP
    out_rows, out_cols = rows_out * TP, sw * DP

    def stage_l(m):
        kind, l = mats[m]
        both = vfs[kind].at[l]
        wait_bytes(both.at[0], v_recv.at[0])
        acc = jnp.concatenate([both[0], both[1]], axis=1)
        own = ts.at[m, t]
        own[:, pl.ds(0, LANES)] = short[pl.ds(m, 1), :]
        if kind == 0:
            col_sum = acc[:, :cols_in]
            oc_in[pl.ds(l, 1), :] = b2 * vc_in[pl.ds(l, 1), :] + (1.0 - b2) * (col_sum / in_rows)
            plane = jnp.sum(col_sum / in_rows, axis=1, keepdims=True)
            olds[pl.ds(l, 1), :] = acc[:, cols_in:cols_in + LANES]
        else:
            r_new = b2 * vr_out[pl.ds(l, 1), :] + (1.0 - b2) * (acc / out_cols)
            or_out[pl.ds(l, 1), :] = r_new
            plane = jnp.sum(r_new, axis=1, keepdims=True)
        own[:, pl.ds(LANES, LANES)] = jnp.broadcast_to(plane, (1, LANES))
        send_tp(ts.at[m], v_send.at[0], v_recv.at[1])

    def stage_e(m):
        kind, l = mats[m]
        wait_bytes(ts.at[m, pl.ds(0, TP - 1)], v_recv.at[1])
        acc = sum_slots(ts.at[m], TP)
        vec = acc[:, :LANES]
        tot = acc[:, LANES:LANES + 1]
        shard = gms[kind].at[l, k_own]
        if kind == 0:
            r_new = b2 * vr_in[pl.ds(l, 1), :] + (1.0 - b2) * (vec / in_cols)
            or_in[pl.ds(l, 1), :] = r_new
            old = jnp.sum(olds[pl.ds(l, 1), :], axis=1, keepdims=True)
            avg = b2 * (old / in_rows) + (1.0 - b2) * (tot / in_cols)
            rb[pl.ds(0, LANES), :] = to_rows(1.0 / jnp.sqrt(r_new))
            cj = jnp.sqrt(avg) / jnp.sqrt(oc_in[pl.ds(l, 1), :])

            def body(i, acc):
                sl = pl.ds(pl.multiple_of(i * 8, 8), 8)
                u = (shard[sl, :] * rb[sl, 0:1]) * cj
                shard[sl, :] = u
                return acc + u * u

            sq = lax.fori_loop(0, sw // 8, body, jnp.zeros((8, cols_in), F32))
        else:
            c_new = b2 * vc_out[pl.ds(l, 1), :] + (1.0 - b2) * (vec / out_rows)
            oc_out[pl.ds(l, 1), :] = c_new
            avg = tot / out_rows
            cj = jnp.sqrt(avg) / jnp.sqrt(c_new)

            def body(i, acc):
                sl = pl.ds(pl.multiple_of(i * LANES, LANES), LANES)
                ri = to_rows(1.0 / jnp.sqrt(or_out[pl.ds(l, 1), sl]))
                u = (shard[sl, :] * ri) * cj
                shard[sl, :] = u
                return acc + u * u

            sq = lax.fori_loop(0, rows_out // LANES, body, jnp.zeros((LANES, LANES), F32))
        tr.at[m, t][...] = jnp.broadcast_to(total(sq), (1, LANES))
        send_tp(tr.at[m], v_send.at[0], v_recv.at[2])

    def stage_f(m):
        wait_bytes(tr.at[m, pl.ds(0, TP - 1)], v_recv.at[2])
        rp.at[m, core][...] = sum_slots(tr.at[m], TP)
        send_core(rp.at[m], v_send.at[0], v_recv.at[3 + m])

    def stage_n(m):
        wait_bytes(rp.at[m, 0], v_recv.at[3 + m])
        rc.at[m, chip][...] = rp.at[m][0] + rp.at[m][1]
        send_chips(rc.at[m], v_send.at[0], v_recv.at[3 + 2 * n_mats + m])

    def stage_g(m):
        mat = mats[m]
        kind, l = mat
        wait_bytes(rc.at[m, pl.ds(0, 3)], v_recv.at[3 + 2 * n_mats + m])
        size = float(in_rows * in_cols if kind == 0 else out_rows * out_cols)
        rms = jnp.sqrt(sum_slots(rc.at[m], 4) / size)
        scale = (1.0 / jnp.maximum(1.0, rms))[:, 0:1]
        shard = gms[kind].at[l, k_own]
        mom = oms[kind].at[l]
        old = wss[kind].at[l]
        new = full_shard(ows, mat, d)
        if l == 0:
            wait_bytes(oms[kind], pre_sem.at[2 * kind])
            wait_bytes(wss[kind], pre_sem.at[2 * kind + 1])
        step = 16 if kind == 0 else 128

        def body(i, carry):
            sl = pl.ds(pl.multiple_of(i * step, step), step)
            mn = (0.9 * mom[sl, :].astype(F32) + 0.1 * (shard[sl, :] * scale)).astype(jnp.bfloat16)
            mom[sl, :] = mn
            w = old[sl, :]
            new[sl, :] = w - lr * mn.astype(F32) - lr * wd * w
            return carry

        lax.fori_loop(0, shard.shape[0] // step, body, 0)
        q = d
        a = full_view(ows, mat, q, 0, False)
        b = full_view(ows, mat, q, 1, False)
        remote(a, a, a_send.at[kind], p2_recv.at[m], t, dev_y)
        remote(b, b, a_send.at[kind], p2_recv.at[m], t, dev_x)
        remote(a, a, a_send.at[kind], p1_recv.at[m, 0], t, dev_x)
        remote(b, b, a_send.at[kind], p1_recv.at[m, 0], t, dev_y)
        pass_core(m, new)

    def pass_core(m, view):
        kind = mats[m][0]
        remote(view, view, ad_send.at[kind], d2_recv.at[kind], t, dev_c)

    def stage_h(m):
        mat = mats[m]
        kind = mat[0]
        a = full_view(ows, mat, 2 * k_y + core, 0, False)
        b = full_view(ows, mat, 2 * k_x + core, 1, False)
        wait_bytes(gms[kind].at[mat[1], 0], p2_recv.at[m])
        for view, dev in ((a, dev_x), (b, dev_y)):
            if m < n_mats - 1:
                remote(view, view, a_send.at[kind], p1_recv.at[m, 1], t, dev)
            else:
                for p in range(PARTS):
                    remote(sub(view, p), sub(view, p), a_send.at[kind], a2_last.at[p], t, dev)
        pass_core(m, a)
        pass_core(m, b)

    def stage_i(m):
        kind, l = mats[m]
        pair = gms[kind].at[l, 0]
        wait_bytes(pair, p1_recv.at[m, 0])
        pass_core(m, full_view(ows, mats[m], 2 * k_x + core, 0, False))
        pass_core(m, full_view(ows, mats[m], 2 * k_y + core, 1, False))
        views = [full_view(ows, mats[m], 2 * k_d + core, h, False) for h in range(2)]
        if m < n_mats - 1:
            wait_bytes(pair, p1_recv.at[m, 1])
            for view in views:
                pass_core(m, view)
        else:
            for p in range(PARTS):
                wait_bytes(sub(pair, p), a2_last.at[p])
                for view in views:
                    pass_core(m, sub(view, p))

    small = [(r_in, vr_in), (c_in, vc_in), (r_out, vr_out), (c_out, vc_out)]
    barrier = pltpu.get_barrier_semaphore()
    z_low = jnp.minimum(t, 1)
    z_high = jnp.minimum(TP - 1 - t, 1)

    def signal_low(sem):
        @pl.when(t > 0)
        def _():
            pl.semaphore_signal(sem, inc=1, device_id=(t - 1, d), device_id_type=MESH)

    def signal_high(sem):
        @pl.when(t < TP - 1)
        def _():
            pl.semaphore_signal(sem, inc=1, device_id=(t + 1, d), device_id_type=MESH)

    for dev in (dev_x, dev_y, dev_c):
        pl.semaphore_signal(barrier, inc=1, device_id=(t, dev), device_id_type=MESH)
    signal_high(barrier)
    load_first(0, 2)
    load_first(2, 8)
    pl.semaphore_wait(barrier, 3 + z_low)
    swap_first()
    stage_a_first()
    start_loads(1)
    start_swap(1)
    signal_low(z_sem.at[0])
    wait_bytes(gm_in.at[0, pl.ds(0, 2)], d2_recv.at[2])
    keep_first(0)
    stage_a(1)
    for i, (src, dst) in enumerate(small):
        pltpu.make_async_copy(src, dst, ld_sem.at[i]).start()
    for m, (kind, l) in enumerate(mats):
        pltpu.make_async_copy((m_in, m_out)[kind].at[l], oms[kind].at[l], pre_sem.at[2 * kind]).start()
        src = w_in.at[l, pl.ds(pl.multiple_of(d * sw, sw), sw), :] if kind == 0 else w_out.at[l, :, pl.ds(pl.multiple_of(d * LANES, LANES), LANES)]
        pltpu.make_async_copy(src, wss[kind].at[l], pre_sem.at[2 * kind + 1]).start()
    wait_bytes(gm_in.at[0], d2_send.at[2])

    @pl.when(t < TP - 1)
    def _():
        pl.semaphore_wait(z_sem.at[0], 1)

    signal_low(z_sem.at[1])
    signal_high(z_sem.at[1])
    for i, (src, dst) in enumerate(small):
        wait_bytes(dst, ld_sem.at[i])
    order = 's2 b0 a2 s3 b1 c0 k0 a3 b2 c1 k1 d0 l0 e0 f0 n0 b3 c2 k2 g0 d1 l1 e1 f1 n1 c3 k3 d2 l2 h0 e2 f2 n2 g1 i0 d3 l3 e3 f3 n3 h1 g2 i1 h2 g3 i2 h3 i3'
    def stage_s(m):
        start_loads(m)
        start_swap(m)

    stages = dict(s=stage_s, a=stage_a, b=stage_b, c=stage_c, d=stage_d, e=stage_e, f=stage_f, g=stage_g, h=stage_h, i=stage_i, k=stage_k, l=stage_l, n=stage_n)
    pl.semaphore_wait(z_sem.at[1], z_low + z_high)
    signal_low(z_sem.at[2])
    signal_high(z_sem.at[2])
    pl.semaphore_wait(z_sem.at[2], z_low + z_high)
    for item in order.split():
        stages[item[0]](int(item[1]))
    for kind in range(2):
        gm = gms[kind]
        wait_bytes(gm, d2_recv.at[kind])
        wait_bytes(gm.at[pl.ds(0, n_layers - 1 + kind)], d2_send.at[kind])
        wait_bytes(r1s[kind], p1_send.at[kind])
        wait_bytes(r2s[kind], p2_send.at[kind])
        wait_bytes(gm.at[:, pl.ds(0, 3)], a_send.at[kind])
        wait_bytes(gm, ad_send.at[kind])
    sizes = [n_layers * (vps[k].shape[3] + (3 + 1) * vhs[k].shape[3]) for k in range(2)]
    sent = sum(sizes) + n_mats * ((TP - 1) * 3 + 1 + 3) * LANES
    wait_bytes(gm_out.at[0, 0, pl.ds(0, sent // LANES)], v_send.at[0])


def store_kernel(*refs):
    n = (len(refs) - 1) // 2
    sems = refs[-1]
    for i in range(n):
        src, dst = refs[i], refs[n + i]
        if i < 2:
            rows = src.shape[1] // STORES
            for l in range(src.shape[0]):
                for c in range(STORES):
                    pltpu.make_async_copy(src.at[l, pl.ds(c * rows, rows)], dst.at[l, pl.ds(c * rows, rows)], sems.at[i]).start()
        else:
            pltpu.make_async_copy(src, dst, sems.at[i]).start()
    for i in range(n):
        pltpu.make_async_copy(refs[i], refs[n + i], sems.at[i]).wait()


def local_step(w_in, w_out, g_in, g_out, m_in, m_out, r_in, c_in, r_out, c_out, lr, wd, b2):
    n_l, rows_in, cols_in = w_in.shape
    rows_out = w_out.shape[1]
    sw = rows_in // DP
    n_m = 2 * n_l
    vec = (cols_in + LANES + 2 * LANES - 1) // (2 * LANES) * (2 * LANES)
    hbm = pl.BlockSpec(memory_space=pltpu.HBM)
    vmem = pl.BlockSpec(memory_space=pltpu.VMEM)
    smem = pl.BlockSpec(memory_space=pltpu.SMEM)
    vm = pltpu.VMEM
    sem = pltpu.SemaphoreType.DMA
    outs = (w_in, w_out, m_in, m_out, r_in, c_in, r_out, c_out)
    res = pl.pallas_call(
        fused_kernel,
        out_shape=tuple(vm(a.shape, a.dtype) for a in outs),
        in_specs=[hbm] * 10 + [smem] * 3,
        out_specs=[vmem] * 8,
        scratch_shapes=[
            vm((n_l, 4, sw, cols_in), F32), vm((n_l, 4, rows_out, LANES), F32),
            vm((n_l, 2, 2, sw // 2, cols_in), F32), vm((n_l, 2, 2, rows_out // 2, LANES), F32),
            vm((n_l, 2, sw // 2, cols_in), F32), vm((n_l, 2, rows_out // 2, LANES), F32),
            vm((n_l, sw, cols_in), F32), vm((n_l, rows_out, LANES), F32),
            vm(r_in.shape, F32), vm(c_in.shape, F32), vm(r_out.shape, F32), vm(c_out.shape, F32),
            vm((n_l + 1, 2, 1, vec), F32), vm((n_l + 1, 2, 1, rows_out), F32),
            vm((n_l + 1, 4, 1, vec // 2), F32), vm((n_l + 1, 4, 1, rows_out // 2), F32),
            vm((n_l + 1, 2, 1, vec // 2), F32), vm((n_l + 1, 2, 1, rows_out // 2), F32),
            vm((n_m + 2, TP, 1, 2 * LANES), F32), vm((n_m + 2, TP, 1, LANES), F32),
            vm((n_m + 4, 2, 1, LANES), F32), vm((n_m + 2, 4, 1, LANES), F32),
            vm((8, LANES), F32), vm((8, LANES), F32), vm((LANES, LANES), F32),
            sem((2 + n_m,)), sem((4,)), sem((3,)), sem((PARTS,)), sem((2 + n_m,)),
            sem((2,)), sem((n_m, 2)), sem((2,)), sem((n_m,)),
            sem((2,)), sem((PARTS,)), sem((2,)), sem((1,)), sem((3 + 3 * n_m,)),
            pltpu.SemaphoreType.REGULAR((3,)),
        ],
        compiler_params=pltpu.CompilerParams(collective_id=0, has_side_effects=True, vmem_limit_bytes=34 * 2 ** 20),
        name='fused_update',
    )(g_in, g_out, w_in, w_out, m_in, m_out, r_in, c_in, r_out, c_out, lr.reshape(1), wd.reshape(1), b2.reshape(1))
    return tuple(pl.pallas_call(
        store_kernel,
        out_shape=tuple(jax.ShapeDtypeStruct(a.shape, a.dtype) for a in outs),
        in_specs=[vmem] * 8,
        out_specs=[hbm] * 8,
        scratch_shapes=[sem((8,))],
        compiler_params=pltpu.CompilerParams(vmem_limit_bytes=2 ** 20),
        name='store_out',
    )(*res))


def solution(mesh):
    in_specs = (P(None, None, 'tp'), P(None, 'tp', None), P('dp', None, None, 'tp'), P('dp', None, 'tp', None), P(None, 'dp', 'tp'), P(None, 'tp', 'dp'), P(None, 'dp'), P(None, 'tp'), P(None, 'tp'), P(None, 'dp'), P(), P(), P())
    out_specs = (P(None, None, 'tp'), P(None, 'tp', None), P(None, 'dp', 'tp'), P(None, 'tp', 'dp'), P(None, 'dp'), P(None, 'tp'), P(None, 'tp'), P(None, 'dp'))
    return jax.shard_map(local_step, mesh=mesh, in_specs=in_specs, out_specs=out_specs, check_vma=False)
```

```python
import jax
import jax.numpy as jnp
from jax import lax
from jax.experimental import pallas as pl
from jax.experimental.pallas import tpu as pltpu
from jax.sharding import PartitionSpec as P

MESH = pl.DeviceIdType.MESH
F32 = jnp.float32
LANES = 128
TP, DP = 4, 8
FIRST = (1, 1, 2, 4)
LAST = (4, 2, 1, 1)
PARTS = 4
STORES = 8


def total(x):
    return jnp.sum(jnp.sum(x, axis=0, keepdims=True), axis=1, keepdims=True)


def eye_mask():
    row = lax.broadcasted_iota(jnp.int32, (LANES, LANES), 0)
    col = lax.broadcasted_iota(jnp.int32, (LANES, LANES), 1)
    return row == col


def to_row(col):
    return jnp.sum(jnp.where(eye_mask(), jnp.broadcast_to(col, (LANES, LANES)), 0.0), axis=0, keepdims=True)


def to_rows(row):
    col = jnp.sum(jnp.where(eye_mask(), jnp.broadcast_to(row, (LANES, LANES)), 0.0), axis=1, keepdims=True)
    return jnp.broadcast_to(col, (LANES, LANES))


def fused_kernel(g_in, g_out, w_in, w_out, m_in, m_out, r_in, c_in, r_out, c_out, lr_ref, wd_ref, b2_ref,
                 ow_in, ow_out, om_in, om_out, or_in, oc_in, or_out, oc_out,
                 gm_in, gm_out, r1_in, r1_out, r2_in, r2_out, ws_in, ws_out,
                 vr_in, vc_in, vr_out, vc_out, vp_in, vp_out, vh_in, vh_out, vf_in, vf_out, ts, tr, rp, rc, short, olds, rb,
                 ld_sem, pre_sem, d2_send, d2_first, d2_recv, p1_send, p1_recv, p2_send, p2_recv,
                 a_send, a2_last, ad_send, v_send, v_recv, z_sem):
    t = lax.axis_index('tp')
    d = lax.axis_index('dp')
    core = lax.rem(d, 2)
    chip = d // 2
    x = lax.rem(chip, 2)
    y = chip // 2
    k_own = chip
    k_x = y * 2 + (1 - x)
    k_y = (1 - y) * 2 + x
    k_d = (1 - y) * 2 + (1 - x)
    dev_x = k_x * 2 + core
    dev_y = k_y * 2 + core
    dev_d = k_d * 2 + core
    dev_c = chip * 2 + (1 - core)
    lr = lr_ref[0]
    wd = wd_ref[0]
    b2 = b2_ref[0]
    n_layers = gm_in.shape[0]
    mats = [(0, i) for i in range(n_layers)] + [(1, i) for i in range(n_layers)]
    n_mats = len(mats)
    sw = gm_in.shape[2]
    half_in = sw // 2
    first = half_in * FIRST[0] // sum(FIRST)
    cols_in = gm_in.shape[3]
    rows_out = gm_out.shape[2]
    half_out = rows_out // 2

    def full_view(refs, mat, q, h, lead):
        kind, l = mat
        pre = (0,) if lead else ()
        if kind == 0:
            return refs[0].at[pre + (l, pl.ds(pl.multiple_of(q * sw + h * half_in, half_in), half_in), slice(None))]
        return refs[1].at[pre + (l, pl.ds(h * half_out, half_out), pl.ds(pl.multiple_of(q * LANES, LANES), LANES))]

    def full_shard(refs, mat, q):
        kind, l = mat
        if kind == 0:
            return refs[0].at[l, pl.ds(pl.multiple_of(q * sw, sw), sw), :]
        return refs[1].at[l, :, pl.ds(pl.multiple_of(q * LANES, LANES), LANES)]

    def half_view(refs, mat, k, h):
        kind, l = mat
        size = half_in if kind == 0 else half_out
        return refs[kind].at[l, k, pl.ds(h * size, size)]

    gs = (g_in, g_out)
    ows = (ow_in, ow_out)
    gms = (gm_in, gm_out)
    r1s = (r1_in, r1_out)
    r2s = (r2_in, r2_out)
    oms = (om_in, om_out)
    wss = (ws_in, ws_out)

    def remote(src, dst, send, recv, dev_t, dev_d):
        cp = pltpu.make_async_remote_copy(src_ref=src, dst_ref=dst, send_sem=send, recv_sem=recv,
                                          device_id=(dev_t, dev_d), device_id_type=MESH)
        cp.start()
        return cp

    def wait_bytes(ref, sem):
        pltpu.make_async_copy(ref, ref, sem).wait()

    def add_into(dst, src):
        rows, cols = dst.shape
        step = 8 if cols > LANES else 128
        if rows % step:
            step = 8

        def body(i, carry):
            sl = pl.ds(pl.multiple_of(i * step, step), step)
            dst[sl, :] = dst[sl, :] + src[sl, :]
            return carry

        lax.fori_loop(0, rows // step, body, 0)

    pieces = [(k_d, 0), (k_d, 1), (k_x, 0), (k_y, 1), (k_y, 0), (k_x, 1), (k_own, 0), (k_own, 1)]
    routes = [(0, 1, dev_x), (1, 1, dev_y), (0, 0, dev_x), (1, 0, dev_y)]

    def sub(ref, i, plan=FIRST):
        unit = ref.shape[0] // sum(plan)
        return ref.at[pl.ds(sum(plan[:i]) * unit, plan[i] * unit)]

    def start_loads(m):
        mat = mats[m]
        for k, h in pieces:
            pltpu.make_async_copy(full_view(gs, mat, 2 * k + core, h, True), half_view(gms, mat, k, h), ld_sem.at[2 + m]).start()

    def load_first():
        def views(i):
            k, h = pieces[i]
            q, mine = 2 * k + (1 - core), 2 * k + core
            return ((full_view(gs, mats[0], q, h, True), full_view(ows, mats[0], q, h, False), pre_sem),
                    (full_view(gs, mats[0], mine, h, True), half_view(gms, mats[0], k, h), ld_sem))

        for step in range(2):
            for which in range(2):
                for i in range(2):
                    src, dst, sem = views(i)[which]
                    rows = pl.ds(0, first) if step == 0 else pl.ds(first, half_in - first)
                    pltpu.make_async_copy(src.at[rows], dst.at[rows], sem.at[step]).start()
        for i in range(2, 8):
            for src, dst, sem in views(i):
                pltpu.make_async_copy(src, dst, sem.at[2]).start()

    def first_bytes(step):
        return gm_in.at[0, 0, pl.ds(0, 2 * first if step == 0 else 2 * (half_in - first))]

    def swap_first():
        views = [full_view(ows, mats[0], 2 * k + (1 - core), h, False) for k, h in pieces]
        for p in range(PARTS):
            if p < 2:
                wait_bytes(first_bytes(p), pre_sem.at[p])
            for i in range(2):
                remote(sub(views[i], p), sub(views[i], p), d2_send.at[2], d2_first.at[p], t, dev_c)

    def swap_rest():
        views = [full_view(ows, mats[0], 2 * k + (1 - core), h, False) for k, h in pieces]
        wait_bytes(gm_in.at[0, pl.ds(0, 3)], pre_sem.at[2])
        for i in range(2, 8):
            remote(views[i], views[i], d2_send.at[2], d2_recv.at[min(i - 2, 2)], t, dev_c)

    def start_swap(m):
        mat = mats[m]
        for k, h in pieces:
            q = 2 * k + (1 - core)
            remote(full_view(gs, mat, q, h, True), full_view(ows, mat, q, h, False), d2_send.at[mat[0]], d2_recv.at[2 + m], t, dev_c)

    def chip_views(m, i):
        k, h = pieces[i]
        return half_view(gms, mats[m], k, h), full_view(ows, mats[m], 2 * k + core, h, False)

    def send_first(m, i, part=None):
        kind, l = mats[m]
        h, j, dev = routes[i]
        mine, other = chip_views(m, i)
        dst = r1s[kind].at[l, h, j]
        if part is not None:
            mine, other, dst = sub(mine, part), sub(other, part), sub(dst, part)
        add_into(mine, other)
        remote(mine, dst, p1_send.at[kind], p1_recv.at[m, j], t, dev)

    def stage_a_first():
        views = [chip_views(0, i)[0] for i in range(8)]
        for p in range(PARTS):
            if p < 2:
                wait_bytes(first_bytes(p), ld_sem.at[p])
            wait_bytes(sub(gm_in.at[0, 0], p), d2_first.at[p])
            for i in range(2):
                send_first(0, i, p)
        swap_rest()
        wait_bytes(gm_in.at[0, pl.ds(0, 3)], ld_sem.at[2])
        for i in range(2, 4):
            wait_bytes(views[i], d2_recv.at[i - 2])
            send_first(0, i)

    def keep_first(m):
        for i in range(4, 8):
            add_into(*chip_views(m, i))

    def stage_a(m):
        kind, l = mats[m]
        gm = gms[kind].at[l]
        wait_bytes(gm, ld_sem.at[2 + m])
        wait_bytes(gm, d2_recv.at[2 + m])
        for i in range(4):
            send_first(m, i)
        keep_first(m)

    def stage_b(m):
        kind, l = mats[m]
        pair = gms[kind].at[l, 0]
        wait_bytes(pair, p1_recv.at[m, 1])
        for h, k, dev in ((0, k_y, dev_y), (1, k_x, dev_x)):
            mine = half_view(gms, mats[m], k, h)
            add_into(mine, r1s[kind].at[l, h, 1])
            remote(mine, r2s[kind].at[l, h], p2_send.at[kind], p2_recv.at[m], t, dev)
        wait_bytes(pair, p1_recv.at[m, 0])
        for h in range(2):
            add_into(half_view(gms, mats[m], k_own, h), r1s[kind].at[l, h, 0])

    vps = (vp_in, vp_out)
    vhs = (vh_in, vh_out)
    vfs = (vf_in, vf_out)

    def send_chips(slots, send, recv):
        for dev in (dev_x, dev_y, dev_d):
            remote(slots.at[chip], slots.at[chip], send, recv, t, dev)

    def send_core(slots, send, recv):
        remote(slots.at[core], slots.at[core], send, recv, t, dev_c)

    def send_tp(slots, send, recv):
        for i in range(1, TP):
            remote(slots.at[t], slots.at[t], send, recv, lax.rem(t + i, TP), d)

    def sum_slots(slots, count):
        acc = slots[0]
        for i in range(1, count):
            acc = acc + slots[i]
        return acc

    def stage_c(m):
        kind, l = mats[m]
        mat = mats[m]
        wait_bytes(gms[kind].at[l, 0], p2_recv.at[m])
        for h in range(2):
            add_into(half_view(gms, mat, k_own, h), r2s[kind].at[l, h])
        own = vps[kind].at[l, core]
        shard = gms[kind].at[l, k_own]
        if kind == 0:
            def body(i, acc):
                sl = pl.ds(pl.multiple_of(i * 8, 8), 8)
                g = shard[sl, :]
                s = g * g + 1e-30
                rb[sl, :] = jnp.broadcast_to(jnp.sum(s, axis=1, keepdims=True), (8, LANES))
                return acc + s

            acc = lax.fori_loop(0, sw // 8, body, jnp.zeros((8, cols_in), F32))
            own[:, pl.ds(0, cols_in)] = jnp.sum(acc, axis=0, keepdims=True)
            own[:, pl.ds(cols_in, LANES)] = vr_in[pl.ds(l, 1), :]
            spare = own.shape[1] - cols_in - LANES
            if spare:
                own[:, pl.ds(cols_in + LANES, spare)] = jnp.zeros((1, spare), F32)
            short[pl.ds(m, 1), :] = to_row(rb[pl.ds(0, LANES), 0:1])
        else:
            def body(i, acc):
                g = shard[pl.ds(pl.multiple_of(i * LANES, LANES), LANES), :]
                s = g * g + 1e-30
                own[:, pl.ds(pl.multiple_of(i * LANES, LANES), LANES)] = to_row(jnp.sum(s, axis=1, keepdims=True))
                return acc + jnp.sum(s, axis=0, keepdims=True)

            short[pl.ds(m, 1), :] = lax.fori_loop(0, rows_out // LANES, body, jnp.zeros((1, LANES), F32))
        send_core(vps[kind].at[l], v_send.at[0], v_recv.at[3 + m])

    def stage_k(m):
        kind, l = mats[m]
        both = vps[kind].at[l]
        wait_bytes(both.at[0], v_recv.at[3 + m])
        size = vhs[kind].shape[3]
        half = pl.ds(pl.multiple_of(core * size, LANES), size)
        vhs[kind].at[l, chip][...] = both.at[0][:, half] + both.at[1][:, half]
        send_chips(vhs[kind].at[l], v_send.at[0], v_recv.at[3 + n_mats + m])

    def stage_d(m):
        kind, l = mats[m]
        slots = vhs[kind].at[l]
        wait_bytes(slots.at[pl.ds(0, 3)], v_recv.at[3 + n_mats + m])
        vfs[kind].at[l, core][...] = sum_slots(slots, 4)
        send_core(vfs[kind].at[l], v_send.at[0], v_recv.at[0])

    in_rows, in_cols = sw * DP, cols_in * TP
    out_rows, out_cols = rows_out * TP, sw * DP

    def stage_l(m):
        kind, l = mats[m]
        both = vfs[kind].at[l]
        wait_bytes(both.at[0], v_recv.at[0])
        acc = jnp.concatenate([both[0], both[1]], axis=1)
        own = ts.at[m, t]
        own[:, pl.ds(0, LANES)] = short[pl.ds(m, 1), :]
        if kind == 0:
            col_sum = acc[:, :cols_in]
            oc_in[pl.ds(l, 1), :] = b2 * vc_in[pl.ds(l, 1), :] + (1.0 - b2) * (col_sum / in_rows)
            plane = jnp.sum(col_sum / in_rows, axis=1, keepdims=True)
            olds[pl.ds(l, 1), :] = acc[:, cols_in:cols_in + LANES]
        else:
            r_new = b2 * vr_out[pl.ds(l, 1), :] + (1.0 - b2) * (acc / out_cols)
            or_out[pl.ds(l, 1), :] = r_new
            plane = jnp.sum(r_new, axis=1, keepdims=True)
        own[:, pl.ds(LANES, LANES)] = jnp.broadcast_to(plane, (1, LANES))
        send_tp(ts.at[m], v_send.at[0], v_recv.at[1])

    def stage_e(m):
        kind, l = mats[m]
        wait_bytes(ts.at[m, pl.ds(0, TP - 1)], v_recv.at[1])
        acc = sum_slots(ts.at[m], TP)
        vec = acc[:, :LANES]
        tot = acc[:, LANES:LANES + 1]
        shard = gms[kind].at[l, k_own]
        if kind == 0:
            r_new = b2 * vr_in[pl.ds(l, 1), :] + (1.0 - b2) * (vec / in_cols)
            or_in[pl.ds(l, 1), :] = r_new
            old = jnp.sum(olds[pl.ds(l, 1), :], axis=1, keepdims=True)
            avg = b2 * (old / in_rows) + (1.0 - b2) * (tot / in_cols)
            rb[pl.ds(0, LANES), :] = to_rows(1.0 / jnp.sqrt(r_new))
            cj = jnp.sqrt(avg) / jnp.sqrt(oc_in[pl.ds(l, 1), :])

            def body(i, acc):
                sl = pl.ds(pl.multiple_of(i * 8, 8), 8)
                u = (shard[sl, :] * rb[sl, 0:1]) * cj
                shard[sl, :] = u
                return acc + u * u

            sq = lax.fori_loop(0, sw // 8, body, jnp.zeros((8, cols_in), F32))
        else:
            c_new = b2 * vc_out[pl.ds(l, 1), :] + (1.0 - b2) * (vec / out_rows)
            oc_out[pl.ds(l, 1), :] = c_new
            avg = tot / out_rows
            cj = jnp.sqrt(avg) / jnp.sqrt(c_new)

            def body(i, acc):
                sl = pl.ds(pl.multiple_of(i * LANES, LANES), LANES)
                ri = to_rows(1.0 / jnp.sqrt(or_out[pl.ds(l, 1), sl]))
                u = (shard[sl, :] * ri) * cj
                shard[sl, :] = u
                return acc + u * u

            sq = lax.fori_loop(0, rows_out // LANES, body, jnp.zeros((LANES, LANES), F32))
        tr.at[m, t][...] = jnp.broadcast_to(total(sq), (1, LANES))
        send_tp(tr.at[m], v_send.at[0], v_recv.at[2])

    def stage_f(m):
        wait_bytes(tr.at[m, pl.ds(0, TP - 1)], v_recv.at[2])
        rp.at[m, core][...] = sum_slots(tr.at[m], TP)
        send_core(rp.at[m], v_send.at[0], v_recv.at[3 + m])

    def stage_n(m):
        wait_bytes(rp.at[m, 0], v_recv.at[3 + m])
        rc.at[m, chip][...] = rp.at[m][0] + rp.at[m][1]
        send_chips(rc.at[m], v_send.at[0], v_recv.at[3 + 2 * n_mats + m])

    def stage_g(m):
        mat = mats[m]
        kind, l = mat
        wait_bytes(rc.at[m, pl.ds(0, 3)], v_recv.at[3 + 2 * n_mats + m])
        size = float(in_rows * in_cols if kind == 0 else out_rows * out_cols)
        rms = jnp.sqrt(sum_slots(rc.at[m], 4) / size)
        scale = (1.0 / jnp.maximum(1.0, rms))[:, 0:1]
        shard = gms[kind].at[l, k_own]
        mom = oms[kind].at[l]
        old = wss[kind].at[l]
        new = full_shard(ows, mat, d)
        if l == 0:
            wait_bytes(oms[kind], pre_sem.at[2 * kind])
            wait_bytes(wss[kind], pre_sem.at[2 * kind + 1])
        step = 16 if kind == 0 else 128

        def body(i, carry):
            sl = pl.ds(pl.multiple_of(i * step, step), step)
            mn = (0.9 * mom[sl, :].astype(F32) + 0.1 * (shard[sl, :] * scale)).astype(jnp.bfloat16)
            mom[sl, :] = mn
            w = old[sl, :]
            new[sl, :] = w - lr * mn.astype(F32) - lr * wd * w
            return carry

        lax.fori_loop(0, shard.shape[0] // step, body, 0)
        q = d
        a = full_view(ows, mat, q, 0, False)
        b = full_view(ows, mat, q, 1, False)
        remote(a, a, a_send.at[kind], p2_recv.at[m], t, dev_y)
        remote(b, b, a_send.at[kind], p2_recv.at[m], t, dev_x)
        remote(a, a, a_send.at[kind], p1_recv.at[m, 0], t, dev_x)
        remote(b, b, a_send.at[kind], p1_recv.at[m, 0], t, dev_y)
        pass_core(m, new)

    def pass_core(m, view):
        kind = mats[m][0]
        remote(view, view, ad_send.at[kind], d2_recv.at[kind], t, dev_c)

    def stage_h(m):
        mat = mats[m]
        kind = mat[0]
        a = full_view(ows, mat, 2 * k_y + core, 0, False)
        b = full_view(ows, mat, 2 * k_x + core, 1, False)
        wait_bytes(gms[kind].at[mat[1], 0], p2_recv.at[m])
        for view, dev in ((a, dev_x), (b, dev_y)):
            if m < n_mats - 1:
                remote(view, view, a_send.at[kind], p1_recv.at[m, 1], t, dev)
            else:
                for p in range(PARTS):
                    part = sub(view, p, LAST)
                    remote(part, part, a_send.at[kind], a2_last.at[p], t, dev)
        pass_core(m, a)
        pass_core(m, b)

    def stage_i(m):
        kind, l = mats[m]
        pair = gms[kind].at[l, 0]
        wait_bytes(pair, p1_recv.at[m, 0])
        pass_core(m, full_view(ows, mats[m], 2 * k_x + core, 0, False))
        pass_core(m, full_view(ows, mats[m], 2 * k_y + core, 1, False))
        views = [full_view(ows, mats[m], 2 * k_d + core, h, False) for h in range(2)]
        if m < n_mats - 1:
            wait_bytes(pair, p1_recv.at[m, 1])
            for view in views:
                pass_core(m, view)
        else:
            for p in range(PARTS):
                wait_bytes(sub(pair, p, LAST), a2_last.at[p])
                for view in views:
                    pass_core(m, sub(view, p, LAST))

    small = [(r_in, vr_in), (c_in, vc_in), (r_out, vr_out), (c_out, vc_out)]
    barrier = pltpu.get_barrier_semaphore()
    z_low = jnp.minimum(t, 1)
    z_high = jnp.minimum(TP - 1 - t, 1)

    def signal_low(sem):
        @pl.when(t > 0)
        def _():
            pl.semaphore_signal(sem, inc=1, device_id=(t - 1, d), device_id_type=MESH)

    def signal_high(sem):
        @pl.when(t < TP - 1)
        def _():
            pl.semaphore_signal(sem, inc=1, device_id=(t + 1, d), device_id_type=MESH)

    for dev in (dev_x, dev_y, dev_c):
        pl.semaphore_signal(barrier, inc=1, device_id=(t, dev), device_id_type=MESH)
    signal_high(barrier)
    load_first()
    pl.semaphore_wait(barrier, 3 + z_low)
    swap_first()
    stage_a_first()
    start_loads(1)
    start_swap(1)
    signal_low(z_sem.at[0])
    wait_bytes(gm_in.at[0, pl.ds(0, 2)], d2_recv.at[2])
    keep_first(0)
    stage_a(1)
    for i, (src, dst) in enumerate(small):
        pltpu.make_async_copy(src, dst, ld_sem.at[i]).start()
    for m, (kind, l) in enumerate(mats):
        pltpu.make_async_copy((m_in, m_out)[kind].at[l], oms[kind].at[l], pre_sem.at[2 * kind]).start()
        src = w_in.at[l, pl.ds(pl.multiple_of(d * sw, sw), sw), :] if kind == 0 else w_out.at[l, :, pl.ds(pl.multiple_of(d * LANES, LANES), LANES)]
        pltpu.make_async_copy(src, wss[kind].at[l], pre_sem.at[2 * kind + 1]).start()
    wait_bytes(gm_in.at[0], d2_send.at[2])

    @pl.when(t < TP - 1)
    def _():
        pl.semaphore_wait(z_sem.at[0], 1)

    signal_low(z_sem.at[1])
    signal_high(z_sem.at[1])
    for i, (src, dst) in enumerate(small):
        wait_bytes(dst, ld_sem.at[i])
    order = 's2 b0 a2 s3 b1 c0 k0 a3 b2 c1 k1 d0 l0 e0 f0 n0 b3 c2 k2 g0 d1 l1 e1 f1 n1 c3 k3 d2 l2 h0 e2 f2 n2 g1 i0 d3 l3 e3 f3 n3 h1 g2 i1 h2 g3 i2 h3 i3'
    def stage_s(m):
        start_loads(m)
        start_swap(m)

    stages = dict(s=stage_s, a=stage_a, b=stage_b, c=stage_c, d=stage_d, e=stage_e, f=stage_f, g=stage_g, h=stage_h, i=stage_i, k=stage_k, l=stage_l, n=stage_n)
    pl.semaphore_wait(z_sem.at[1], z_low + z_high)
    signal_low(z_sem.at[2])
    signal_high(z_sem.at[2])
    pl.semaphore_wait(z_sem.at[2], z_low + z_high)
    for item in order.split():
        stages[item[0]](int(item[1]))
    for kind in range(2):
        gm = gms[kind]
        wait_bytes(gm, d2_recv.at[kind])
        wait_bytes(gm.at[pl.ds(0, n_layers - 1 + kind)], d2_send.at[kind])
        wait_bytes(r1s[kind], p1_send.at[kind])
        wait_bytes(r2s[kind], p2_send.at[kind])
        wait_bytes(gm.at[:, pl.ds(0, 3)], a_send.at[kind])
        wait_bytes(gm, ad_send.at[kind])
    sizes = [n_layers * (vps[k].shape[3] + (3 + 1) * vhs[k].shape[3]) for k in range(2)]
    sent = sum(sizes) + n_mats * ((TP - 1) * 3 + 1 + 3) * LANES
    wait_bytes(gm_out.at[0, 0, pl.ds(0, sent // LANES)], v_send.at[0])


def store_kernel(*refs):
    n = (len(refs) - 1) // 2
    sems = refs[-1]
    for i in range(n):
        src, dst = refs[i], refs[n + i]
        if i < 2:
            rows = src.shape[1] // STORES
            for l in range(src.shape[0]):
                for c in range(STORES):
                    pltpu.make_async_copy(src.at[l, pl.ds(c * rows, rows)], dst.at[l, pl.ds(c * rows, rows)], sems.at[i]).start()
        else:
            pltpu.make_async_copy(src, dst, sems.at[i]).start()
    for i in range(n):
        pltpu.make_async_copy(refs[i], refs[n + i], sems.at[i]).wait()


def local_step(w_in, w_out, g_in, g_out, m_in, m_out, r_in, c_in, r_out, c_out, lr, wd, b2):
    n_l, rows_in, cols_in = w_in.shape
    rows_out = w_out.shape[1]
    sw = rows_in // DP
    n_m = 2 * n_l
    vec = (cols_in + LANES + 2 * LANES - 1) // (2 * LANES) * (2 * LANES)
    hbm = pl.BlockSpec(memory_space=pltpu.HBM)
    vmem = pl.BlockSpec(memory_space=pltpu.VMEM)
    smem = pl.BlockSpec(memory_space=pltpu.SMEM)
    vm = pltpu.VMEM
    sem = pltpu.SemaphoreType.DMA
    outs = (w_in, w_out, m_in, m_out, r_in, c_in, r_out, c_out)
    res = pl.pallas_call(
        fused_kernel,
        out_shape=tuple(vm(a.shape, a.dtype) for a in outs),
        in_specs=[hbm] * 10 + [smem] * 3,
        out_specs=[vmem] * 8,
        scratch_shapes=[
            vm((n_l, 4, sw, cols_in), F32), vm((n_l, 4, rows_out, LANES), F32),
            vm((n_l, 2, 2, sw // 2, cols_in), F32), vm((n_l, 2, 2, rows_out // 2, LANES), F32),
            vm((n_l, 2, sw // 2, cols_in), F32), vm((n_l, 2, rows_out // 2, LANES), F32),
            vm((n_l, sw, cols_in), F32), vm((n_l, rows_out, LANES), F32),
            vm(r_in.shape, F32), vm(c_in.shape, F32), vm(r_out.shape, F32), vm(c_out.shape, F32),
            vm((n_l + 1, 2, 1, vec), F32), vm((n_l + 1, 2, 1, rows_out), F32),
            vm((n_l + 1, 4, 1, vec // 2), F32), vm((n_l + 1, 4, 1, rows_out // 2), F32),
            vm((n_l + 1, 2, 1, vec // 2), F32), vm((n_l + 1, 2, 1, rows_out // 2), F32),
            vm((n_m + 2, TP, 1, 2 * LANES), F32), vm((n_m + 2, TP, 1, LANES), F32),
            vm((n_m + 4, 2, 1, LANES), F32), vm((n_m + 2, 4, 1, LANES), F32),
            vm((8, LANES), F32), vm((8, LANES), F32), vm((LANES, LANES), F32),
            sem((2 + n_m,)), sem((4,)), sem((3,)), sem((PARTS,)), sem((2 + n_m,)),
            sem((2,)), sem((n_m, 2)), sem((2,)), sem((n_m,)),
            sem((2,)), sem((PARTS,)), sem((2,)), sem((1,)), sem((3 + 3 * n_m,)),
            pltpu.SemaphoreType.REGULAR((3,)),
        ],
        compiler_params=pltpu.CompilerParams(collective_id=0, has_side_effects=True, vmem_limit_bytes=34 * 2 ** 20),
        name='fused_update',
    )(g_in, g_out, w_in, w_out, m_in, m_out, r_in, c_in, r_out, c_out, lr.reshape(1), wd.reshape(1), b2.reshape(1))
    return tuple(pl.pallas_call(
        store_kernel,
        out_shape=tuple(jax.ShapeDtypeStruct(a.shape, a.dtype) for a in outs),
        in_specs=[vmem] * 8,
        out_specs=[hbm] * 8,
        scratch_shapes=[sem((8,))],
        compiler_params=pltpu.CompilerParams(vmem_limit_bytes=2 ** 20),
        name='store_out',
    )(*res))


def solution(mesh):
    in_specs = (P(None, None, 'tp'), P(None, 'tp', None), P('dp', None, None, 'tp'), P('dp', None, 'tp', None), P(None, 'dp', 'tp'), P(None, 'tp', 'dp'), P(None, 'dp'), P(None, 'tp'), P(None, 'tp'), P(None, 'dp'), P(), P(), P())
    out_specs = (P(None, None, 'tp'), P(None, 'tp', None), P(None, 'dp', 'tp'), P(None, 'tp', 'dp'), P(None, 'dp'), P(None, 'tp'), P(None, 'tp'), P(None, 'dp'))
    return jax.shard_map(local_step, mesh=mesh, in_specs=in_specs, out_specs=out_specs, check_vma=False)
```

```python
import jax
import jax.numpy as jnp
from jax import lax
from jax.experimental import pallas as pl
from jax.experimental.pallas import tpu as pltpu
from jax.sharding import PartitionSpec as P

MESH = pl.DeviceIdType.MESH
F32 = jnp.float32
LANES = 128
TP, DP = 4, 8
FIRST = (1, 1, 2, 4)
LAST = (4, 2, 1, 1)
PARTS = 4
STORES = 8


def total(x):
    return jnp.sum(jnp.sum(x, axis=0, keepdims=True), axis=1, keepdims=True)


def eye_mask():
    row = lax.broadcasted_iota(jnp.int32, (LANES, LANES), 0)
    col = lax.broadcasted_iota(jnp.int32, (LANES, LANES), 1)
    return row == col


def to_row(col):
    return jnp.sum(jnp.where(eye_mask(), jnp.broadcast_to(col, (LANES, LANES)), 0.0), axis=0, keepdims=True)


def to_rows(row):
    col = jnp.sum(jnp.where(eye_mask(), jnp.broadcast_to(row, (LANES, LANES)), 0.0), axis=1, keepdims=True)
    return jnp.broadcast_to(col, (LANES, LANES))


def fused_kernel(g_in, g_out, w_in, w_out, m_in, m_out, r_in, c_in, r_out, c_out, lr_ref, wd_ref, b2_ref,
                 ow_in, ow_out, om_in, om_out, or_in, oc_in, or_out, oc_out,
                 gm_in, gm_out, r1_in, r1_out, r2_in, r2_out, ws_in, ws_out,
                 vr_in, vc_in, vr_out, vc_out, vp_in, vp_out, vh_in, vh_out, vf_in, vf_out, ts, tr, rp, rc, short, olds, rb,
                 ld_sem, pre_sem, d2_send, d2_first, d2_recv, p1_send, p1_recv, p2_send, p2_recv,
                 a2_last, v_send, v_recv, z_sem):
    t = lax.axis_index('tp')
    d = lax.axis_index('dp')
    core = lax.rem(d, 2)
    chip = d // 2
    x = lax.rem(chip, 2)
    y = chip // 2
    k_own = chip
    k_x = y * 2 + (1 - x)
    k_y = (1 - y) * 2 + x
    k_d = (1 - y) * 2 + (1 - x)
    dev_x = k_x * 2 + core
    dev_y = k_y * 2 + core
    dev_d = k_d * 2 + core
    dev_c = chip * 2 + (1 - core)
    lr = lr_ref[0]
    wd = wd_ref[0]
    b2 = b2_ref[0]
    n_layers = gm_in.shape[0]
    mats = [(0, i) for i in range(n_layers)] + [(1, i) for i in range(n_layers)]
    n_mats = len(mats)
    sw = gm_in.shape[2]
    half_in = sw // 2
    first = half_in * FIRST[0] // sum(FIRST)
    cols_in = gm_in.shape[3]
    rows_out = gm_out.shape[2]
    half_out = rows_out // 2

    def full_view(refs, mat, q, h, lead):
        kind, l = mat
        pre = (0,) if lead else ()
        if kind == 0:
            return refs[0].at[pre + (l, pl.ds(pl.multiple_of(q * sw + h * half_in, half_in), half_in), slice(None))]
        return refs[1].at[pre + (l, pl.ds(h * half_out, half_out), pl.ds(pl.multiple_of(q * LANES, LANES), LANES))]

    def full_shard(refs, mat, q):
        kind, l = mat
        if kind == 0:
            return refs[0].at[l, pl.ds(pl.multiple_of(q * sw, sw), sw), :]
        return refs[1].at[l, :, pl.ds(pl.multiple_of(q * LANES, LANES), LANES)]

    def half_view(refs, mat, k, h):
        kind, l = mat
        size = half_in if kind == 0 else half_out
        return refs[kind].at[l, k, pl.ds(h * size, size)]

    gs = (g_in, g_out)
    ows = (ow_in, ow_out)
    gms = (gm_in, gm_out)
    r1s = (r1_in, r1_out)
    r2s = (r2_in, r2_out)
    oms = (om_in, om_out)
    wss = (ws_in, ws_out)

    def remote(src, dst, send, recv, dev_t, dev_d):
        cp = pltpu.make_async_remote_copy(src_ref=src, dst_ref=dst, send_sem=send, recv_sem=recv,
                                          device_id=(dev_t, dev_d), device_id_type=MESH)
        cp.start()
        return cp

    def wait_bytes(ref, sem):
        pltpu.make_async_copy(ref, ref, sem).wait()

    def add_into(dst, src):
        rows, cols = dst.shape
        step = 8 if cols > LANES else 128
        if rows % step:
            step = 8

        def body(i, carry):
            sl = pl.ds(pl.multiple_of(i * step, step), step)
            dst[sl, :] = dst[sl, :] + src[sl, :]
            return carry

        lax.fori_loop(0, rows // step, body, 0)

    pieces = [(k_d, 0), (k_d, 1), (k_x, 0), (k_y, 1), (k_y, 0), (k_x, 1), (k_own, 0), (k_own, 1)]
    routes = [(0, 1, dev_x), (1, 1, dev_y), (0, 0, dev_x), (1, 0, dev_y)]

    def sub(ref, i, plan=FIRST):
        unit = ref.shape[0] // sum(plan)
        return ref.at[pl.ds(sum(plan[:i]) * unit, plan[i] * unit)]

    def start_loads(m):
        mat = mats[m]
        for k, h in pieces:
            pltpu.make_async_copy(full_view(gs, mat, 2 * k + core, h, True), half_view(gms, mat, k, h), ld_sem.at[3]).start()

    def load_first():
        def views(i):
            k, h = pieces[i]
            q, mine = 2 * k + (1 - core), 2 * k + core
            return ((full_view(gs, mats[0], q, h, True), full_view(ows, mats[0], q, h, False), pre_sem),
                    (full_view(gs, mats[0], mine, h, True), half_view(gms, mats[0], k, h), ld_sem))

        for step in range(2):
            for which in range(2):
                for i in range(2):
                    src, dst, sem = views(i)[which]
                    rows = pl.ds(0, first) if step == 0 else pl.ds(first, half_in - first)
                    pltpu.make_async_copy(src.at[rows], dst.at[rows], sem.at[step]).start()
        for i in range(2, 8):
            for src, dst, sem in views(i):
                pltpu.make_async_copy(src, dst, sem.at[2]).start()

    def first_bytes(step):
        return gm_in.at[0, 0, pl.ds(0, 2 * first if step == 0 else 2 * (half_in - first))]

    def swap_first():
        views = [full_view(ows, mats[0], 2 * k + (1 - core), h, False) for k, h in pieces]
        for p in range(PARTS):
            if p < 2:
                wait_bytes(first_bytes(p), pre_sem.at[p])
            for i in range(2):
                remote(sub(views[i], p), sub(views[i], p), d2_send.at[2], d2_first.at[p], t, dev_c)

    def swap_rest():
        views = [full_view(ows, mats[0], 2 * k + (1 - core), h, False) for k, h in pieces]
        wait_bytes(gm_in.at[0, pl.ds(0, 3)], pre_sem.at[2])
        for i in range(2, 8):
            remote(views[i], views[i], d2_send.at[2], d2_recv.at[min(i - 2, 2)], t, dev_c)

    def start_swap(m):
        mat = mats[m]
        for k, h in pieces:
            q = 2 * k + (1 - core)
            remote(full_view(gs, mat, q, h, True), full_view(ows, mat, q, h, False), d2_send.at[mat[0]], d2_recv.at[2 + m], t, dev_c)

    def chip_views(m, i):
        k, h = pieces[i]
        return half_view(gms, mats[m], k, h), full_view(ows, mats[m], 2 * k + core, h, False)

    def send_first(m, i, part=None):
        kind, l = mats[m]
        h, j, dev = routes[i]
        mine, other = chip_views(m, i)
        dst = r1s[kind].at[l, h, j]
        if part is not None:
            mine, other, dst = sub(mine, part), sub(other, part), sub(dst, part)
        add_into(mine, other)
        remote(mine, dst, p1_send.at[kind], p1_recv.at[m, j], t, dev)

    def stage_a_first():
        views = [chip_views(0, i)[0] for i in range(8)]
        for p in range(PARTS):
            if p < 2:
                wait_bytes(first_bytes(p), ld_sem.at[p])
            wait_bytes(sub(gm_in.at[0, 0], p), d2_first.at[p])
            for i in range(2):
                send_first(0, i, p)
        swap_rest()
        wait_bytes(gm_in.at[0, pl.ds(0, 3)], ld_sem.at[2])
        for i in range(2, 4):
            wait_bytes(views[i], d2_recv.at[i - 2])
            send_first(0, i)

    def keep_first(m):
        for i in range(4, 8):
            add_into(*chip_views(m, i))

    def stage_a(m):
        kind, l = mats[m]
        gm = gms[kind].at[l]
        wait_bytes(gm, ld_sem.at[3])
        wait_bytes(gm, d2_recv.at[2 + m])
        for i in range(4):
            send_first(m, i)
        keep_first(m)

    def stage_b(m):
        kind, l = mats[m]
        pair = gms[kind].at[l, 0]
        wait_bytes(pair, p1_recv.at[m, 1])
        for h, k, dev in ((0, k_y, dev_y), (1, k_x, dev_x)):
            mine = half_view(gms, mats[m], k, h)
            add_into(mine, r1s[kind].at[l, h, 1])
            remote(mine, r2s[kind].at[l, h], p2_send.at[kind], p2_recv.at[m], t, dev)
        wait_bytes(pair, p1_recv.at[m, 0])
        for h in range(2):
            add_into(half_view(gms, mats[m], k_own, h), r1s[kind].at[l, h, 0])

    vps = (vp_in, vp_out)
    vhs = (vh_in, vh_out)
    vfs = (vf_in, vf_out)

    def send_chips(slots, send, recv):
        for dev in (dev_x, dev_y, dev_d):
            remote(slots.at[chip], slots.at[chip], send, recv, t, dev)

    def send_core(slots, send, recv):
        remote(slots.at[core], slots.at[core], send, recv, t, dev_c)

    def send_tp(slots, send, recv):
        for i in range(1, TP):
            remote(slots.at[t], slots.at[t], send, recv, lax.rem(t + i, TP), d)

    def sum_slots(slots, count):
        acc = slots[0]
        for i in range(1, count):
            acc = acc + slots[i]
        return acc

    def stage_c(m):
        kind, l = mats[m]
        mat = mats[m]
        wait_bytes(gms[kind].at[l, 0], p2_recv.at[m])
        for h in range(2):
            add_into(half_view(gms, mat, k_own, h), r2s[kind].at[l, h])
        own = vps[kind].at[l, core]
        shard = gms[kind].at[l, k_own]
        if kind == 0:
            def body(i, acc):
                sl = pl.ds(pl.multiple_of(i * 8, 8), 8)
                g = shard[sl, :]
                s = g * g + 1e-30
                rb[sl, :] = jnp.broadcast_to(jnp.sum(s, axis=1, keepdims=True), (8, LANES))
                return acc + s

            acc = lax.fori_loop(0, sw // 8, body, jnp.zeros((8, cols_in), F32))
            own[:, pl.ds(0, cols_in)] = jnp.sum(acc, axis=0, keepdims=True)
            own[:, pl.ds(cols_in, LANES)] = vr_in[pl.ds(l, 1), :]
            spare = own.shape[1] - cols_in - LANES
            if spare:
                own[:, pl.ds(cols_in + LANES, spare)] = jnp.zeros((1, spare), F32)
            short[pl.ds(m, 1), :] = to_row(rb[pl.ds(0, LANES), 0:1])
        else:
            def body(i, acc):
                g = shard[pl.ds(pl.multiple_of(i * LANES, LANES), LANES), :]
                s = g * g + 1e-30
                own[:, pl.ds(pl.multiple_of(i * LANES, LANES), LANES)] = to_row(jnp.sum(s, axis=1, keepdims=True))
                return acc + jnp.sum(s, axis=0, keepdims=True)

            short[pl.ds(m, 1), :] = lax.fori_loop(0, rows_out // LANES, body, jnp.zeros((1, LANES), F32))
        send_core(vps[kind].at[l], v_send.at[0], v_recv.at[3 + m])

    def stage_k(m):
        kind, l = mats[m]
        both = vps[kind].at[l]
        wait_bytes(both.at[0], v_recv.at[3 + m])
        size = vhs[kind].shape[3]
        half = pl.ds(pl.multiple_of(core * size, LANES), size)
        vhs[kind].at[l, chip][...] = both.at[0][:, half] + both.at[1][:, half]
        send_chips(vhs[kind].at[l], v_send.at[0], v_recv.at[3 + n_mats + m])

    def stage_d(m):
        kind, l = mats[m]
        slots = vhs[kind].at[l]
        wait_bytes(slots.at[pl.ds(0, 3)], v_recv.at[3 + n_mats + m])
        vfs[kind].at[l, core][...] = sum_slots(slots, 4)
        send_core(vfs[kind].at[l], v_send.at[0], v_recv.at[0])

    in_rows, in_cols = sw * DP, cols_in * TP
    out_rows, out_cols = rows_out * TP, sw * DP

    def stage_l(m):
        kind, l = mats[m]
        both = vfs[kind].at[l]
        wait_bytes(both.at[0], v_recv.at[0])
        acc = jnp.concatenate([both[0], both[1]], axis=1)
        own = ts.at[m, t]
        own[:, pl.ds(0, LANES)] = short[pl.ds(m, 1), :]
        if kind == 0:
            col_sum = acc[:, :cols_in]
            oc_in[pl.ds(l, 1), :] = b2 * vc_in[pl.ds(l, 1), :] + (1.0 - b2) * (col_sum / in_rows)
            plane = jnp.sum(col_sum / in_rows, axis=1, keepdims=True)
            olds[pl.ds(l, 1), :] = acc[:, cols_in:cols_in + LANES]
        else:
            r_new = b2 * vr_out[pl.ds(l, 1), :] + (1.0 - b2) * (acc / out_cols)
            or_out[pl.ds(l, 1), :] = r_new
            plane = jnp.sum(r_new, axis=1, keepdims=True)
        own[:, pl.ds(LANES, LANES)] = jnp.broadcast_to(plane, (1, LANES))
        send_tp(ts.at[m], v_send.at[0], v_recv.at[1])

    def stage_e(m):
        kind, l = mats[m]
        wait_bytes(ts.at[m, pl.ds(0, TP - 1)], v_recv.at[1])
        acc = sum_slots(ts.at[m], TP)
        vec = acc[:, :LANES]
        tot = acc[:, LANES:LANES + 1]
        shard = gms[kind].at[l, k_own]
        if kind == 0:
            r_new = b2 * vr_in[pl.ds(l, 1), :] + (1.0 - b2) * (vec / in_cols)
            or_in[pl.ds(l, 1), :] = r_new
            old = jnp.sum(olds[pl.ds(l, 1), :], axis=1, keepdims=True)
            avg = b2 * (old / in_rows) + (1.0 - b2) * (tot / in_cols)
            rb[pl.ds(0, LANES), :] = to_rows(1.0 / jnp.sqrt(r_new))
            cj = jnp.sqrt(avg) / jnp.sqrt(oc_in[pl.ds(l, 1), :])

            def body(i, acc):
                sl = pl.ds(pl.multiple_of(i * 8, 8), 8)
                u = (shard[sl, :] * rb[sl, 0:1]) * cj
                shard[sl, :] = u
                return acc + u * u

            sq = lax.fori_loop(0, sw // 8, body, jnp.zeros((8, cols_in), F32))
        else:
            c_new = b2 * vc_out[pl.ds(l, 1), :] + (1.0 - b2) * (vec / out_rows)
            oc_out[pl.ds(l, 1), :] = c_new
            avg = tot / out_rows
            cj = jnp.sqrt(avg) / jnp.sqrt(c_new)

            def body(i, acc):
                sl = pl.ds(pl.multiple_of(i * LANES, LANES), LANES)
                ri = to_rows(1.0 / jnp.sqrt(or_out[pl.ds(l, 1), sl]))
                u = (shard[sl, :] * ri) * cj
                shard[sl, :] = u
                return acc + u * u

            sq = lax.fori_loop(0, rows_out // LANES, body, jnp.zeros((LANES, LANES), F32))
        tr.at[m, t][...] = jnp.broadcast_to(total(sq), (1, LANES))
        send_tp(tr.at[m], v_send.at[0], v_recv.at[2])

    def stage_f(m):
        wait_bytes(tr.at[m, pl.ds(0, TP - 1)], v_recv.at[2])
        rp.at[m, core][...] = sum_slots(tr.at[m], TP)
        send_core(rp.at[m], v_send.at[0], v_recv.at[3 + m])

    def stage_n(m):
        wait_bytes(rp.at[m, 0], v_recv.at[3 + m])
        rc.at[m, chip][...] = rp.at[m][0] + rp.at[m][1]
        send_chips(rc.at[m], v_send.at[0], v_recv.at[3 + 2 * n_mats + m])

    def stage_g(m):
        mat = mats[m]
        kind, l = mat
        wait_bytes(rc.at[m, pl.ds(0, 3)], v_recv.at[3 + 2 * n_mats + m])
        size = float(in_rows * in_cols if kind == 0 else out_rows * out_cols)
        rms = jnp.sqrt(sum_slots(rc.at[m], 4) / size)
        scale = (1.0 / jnp.maximum(1.0, rms))[:, 0:1]
        shard = gms[kind].at[l, k_own]
        mom = oms[kind].at[l]
        old = wss[kind].at[l]
        new = full_shard(ows, mat, d)
        if l == 0:
            wait_bytes(r1s[kind], p1_send.at[kind])
            wait_bytes(gms[kind].at[pl.ds(0, n_layers - 1 + kind)], d2_send.at[kind])
            wait_bytes(oms[kind], pre_sem.at[2 * kind])
            wait_bytes(wss[kind], pre_sem.at[2 * kind + 1])
        step = 16 if kind == 0 else 128

        def body(i, carry):
            sl = pl.ds(pl.multiple_of(i * step, step), step)
            mn = (0.9 * mom[sl, :].astype(F32) + 0.1 * (shard[sl, :] * scale)).astype(jnp.bfloat16)
            mom[sl, :] = mn
            w = old[sl, :]
            new[sl, :] = w - lr * mn.astype(F32) - lr * wd * w
            return carry

        lax.fori_loop(0, shard.shape[0] // step, body, 0)
        q = d
        a = full_view(ows, mat, q, 0, False)
        b = full_view(ows, mat, q, 1, False)
        remote(a, a, p1_send.at[kind], p2_recv.at[m], t, dev_y)
        remote(b, b, p1_send.at[kind], p2_recv.at[m], t, dev_x)
        remote(a, a, p1_send.at[kind], p1_recv.at[m, 0], t, dev_x)
        remote(b, b, p1_send.at[kind], p1_recv.at[m, 0], t, dev_y)
        pass_core(m, new)

    def pass_core(m, view):
        kind = mats[m][0]
        remote(view, view, d2_send.at[kind], d2_recv.at[kind], t, dev_c)

    def stage_h(m):
        mat = mats[m]
        kind = mat[0]
        a = full_view(ows, mat, 2 * k_y + core, 0, False)
        b = full_view(ows, mat, 2 * k_x + core, 1, False)
        wait_bytes(gms[kind].at[mat[1], 0], p2_recv.at[m])
        for view, dev in ((a, dev_x), (b, dev_y)):
            if m < n_mats - 1:
                remote(view, view, p1_send.at[kind], p1_recv.at[m, 1], t, dev)
            else:
                for p in range(PARTS):
                    part = sub(view, p, LAST)
                    remote(part, part, p1_send.at[kind], a2_last.at[p], t, dev)
        pass_core(m, a)
        pass_core(m, b)

    def stage_i(m):
        kind, l = mats[m]
        pair = gms[kind].at[l, 0]
        wait_bytes(pair, p1_recv.at[m, 0])
        pass_core(m, full_view(ows, mats[m], 2 * k_x + core, 0, False))
        pass_core(m, full_view(ows, mats[m], 2 * k_y + core, 1, False))
        views = [full_view(ows, mats[m], 2 * k_d + core, h, False) for h in range(2)]
        if m < n_mats - 1:
            wait_bytes(pair, p1_recv.at[m, 1])
            for view in views:
                pass_core(m, view)
        else:
            for p in range(PARTS):
                wait_bytes(sub(pair, p, LAST), a2_last.at[p])
                for view in views:
                    pass_core(m, sub(view, p, LAST))

    small = [(r_in, vr_in), (c_in, vc_in), (r_out, vr_out), (c_out, vc_out)]
    barrier = pltpu.get_barrier_semaphore()
    z_low = jnp.minimum(t, 1)
    z_high = jnp.minimum(TP - 1 - t, 1)

    def signal_low(sem):
        @pl.when(t > 0)
        def _():
            pl.semaphore_signal(sem, inc=1, device_id=(t - 1, d), device_id_type=MESH)

    def signal_high(sem):
        @pl.when(t < TP - 1)
        def _():
            pl.semaphore_signal(sem, inc=1, device_id=(t + 1, d), device_id_type=MESH)

    for dev in (dev_x, dev_y, dev_c):
        pl.semaphore_signal(barrier, inc=1, device_id=(t, dev), device_id_type=MESH)
    signal_high(barrier)
    load_first()
    pl.semaphore_wait(barrier, 3 + z_low)
    swap_first()
    stage_a_first()
    start_loads(1)
    start_swap(1)
    signal_low(z_sem.at[0])
    wait_bytes(gm_in.at[0, pl.ds(0, 2)], d2_recv.at[2])
    keep_first(0)
    stage_a(1)
    for i, (src, dst) in enumerate(small):
        pltpu.make_async_copy(src, dst, ld_sem.at[i]).start()
    for m, (kind, l) in enumerate(mats):
        pltpu.make_async_copy((m_in, m_out)[kind].at[l], oms[kind].at[l], pre_sem.at[2 * kind]).start()
        src = w_in.at[l, pl.ds(pl.multiple_of(d * sw, sw), sw), :] if kind == 0 else w_out.at[l, :, pl.ds(pl.multiple_of(d * LANES, LANES), LANES)]
        pltpu.make_async_copy(src, wss[kind].at[l], pre_sem.at[2 * kind + 1]).start()
    wait_bytes(gm_in.at[0], d2_send.at[2])

    @pl.when(t < TP - 1)
    def _():
        pl.semaphore_wait(z_sem.at[0], 1)

    signal_low(z_sem.at[1])
    signal_high(z_sem.at[1])
    for i, (src, dst) in enumerate(small):
        wait_bytes(dst, ld_sem.at[i])
    order = 's2 b0 a2 s3 b1 c0 k0 a3 b2 c1 k1 d0 l0 e0 f0 n0 b3 c2 k2 g0 d1 l1 e1 f1 n1 c3 k3 d2 l2 h0 e2 f2 n2 g1 i0 d3 l3 e3 f3 n3 h1 g2 i1 h2 g3 i2 h3 i3'
    def stage_s(m):
        start_loads(m)
        start_swap(m)

    stages = dict(s=stage_s, a=stage_a, b=stage_b, c=stage_c, d=stage_d, e=stage_e, f=stage_f, g=stage_g, h=stage_h, i=stage_i, k=stage_k, l=stage_l, n=stage_n)
    pl.semaphore_wait(z_sem.at[1], z_low + z_high)
    signal_low(z_sem.at[2])
    signal_high(z_sem.at[2])
    pl.semaphore_wait(z_sem.at[2], z_low + z_high)
    for item in order.split():
        stages[item[0]](int(item[1]))
    for kind in range(2):
        gm = gms[kind]
        wait_bytes(gm, d2_recv.at[kind])
        wait_bytes(r2s[kind], p2_send.at[kind])
        wait_bytes(gm.at[:, pl.ds(0, 3)], p1_send.at[kind])
        wait_bytes(gm, d2_send.at[kind])
    sizes = [n_layers * (vps[k].shape[3] + (3 + 1) * vhs[k].shape[3]) for k in range(2)]
    sent = sum(sizes) + n_mats * ((TP - 1) * 3 + 1 + 3) * LANES
    wait_bytes(gm_out.at[0, 0, pl.ds(0, sent // LANES)], v_send.at[0])


def store_kernel(*refs):
    n = (len(refs) - 1) // 2
    sems = refs[-1]
    for i in range(n):
        src, dst = refs[i], refs[n + i]
        if i < 2:
            rows = src.shape[1] // STORES
            for l in range(src.shape[0]):
                for c in range(STORES):
                    pltpu.make_async_copy(src.at[l, pl.ds(c * rows, rows)], dst.at[l, pl.ds(c * rows, rows)], sems.at[i]).start()
        else:
            pltpu.make_async_copy(src, dst, sems.at[i]).start()
    for i in range(n):
        pltpu.make_async_copy(refs[i], refs[n + i], sems.at[i]).wait()


def local_step(w_in, w_out, g_in, g_out, m_in, m_out, r_in, c_in, r_out, c_out, lr, wd, b2):
    n_l, rows_in, cols_in = w_in.shape
    rows_out = w_out.shape[1]
    sw = rows_in // DP
    n_m = 2 * n_l
    vec = (cols_in + LANES + 2 * LANES - 1) // (2 * LANES) * (2 * LANES)
    hbm = pl.BlockSpec(memory_space=pltpu.HBM)
    vmem = pl.BlockSpec(memory_space=pltpu.VMEM)
    smem = pl.BlockSpec(memory_space=pltpu.SMEM)
    vm = pltpu.VMEM
    sem = pltpu.SemaphoreType.DMA
    outs = (w_in, w_out, m_in, m_out, r_in, c_in, r_out, c_out)
    res = pl.pallas_call(
        fused_kernel,
        out_shape=tuple(vm(a.shape, a.dtype) for a in outs),
        in_specs=[hbm] * 10 + [smem] * 3,
        out_specs=[vmem] * 8,
        scratch_shapes=[
            vm((n_l, 4, sw, cols_in), F32), vm((n_l, 4, rows_out, LANES), F32),
            vm((n_l, 2, 2, sw // 2, cols_in), F32), vm((n_l, 2, 2, rows_out // 2, LANES), F32),
            vm((n_l, 2, sw // 2, cols_in), F32), vm((n_l, 2, rows_out // 2, LANES), F32),
            vm((n_l, sw, cols_in), F32), vm((n_l, rows_out, LANES), F32),
            vm(r_in.shape, F32), vm(c_in.shape, F32), vm(r_out.shape, F32), vm(c_out.shape, F32),
            vm((n_l + 1, 2, 1, vec), F32), vm((n_l + 1, 2, 1, rows_out), F32),
            vm((n_l + 1, 4, 1, vec // 2), F32), vm((n_l + 1, 4, 1, rows_out // 2), F32),
            vm((n_l + 1, 2, 1, vec // 2), F32), vm((n_l + 1, 2, 1, rows_out // 2), F32),
            vm((n_m + 2, TP, 1, 2 * LANES), F32), vm((n_m + 2, TP, 1, LANES), F32),
            vm((n_m + 4, 2, 1, LANES), F32), vm((n_m + 2, 4, 1, LANES), F32),
            vm((8, LANES), F32), vm((8, LANES), F32), vm((LANES, LANES), F32),
            sem((4,)), sem((4,)), sem((3,)), sem((PARTS,)), sem((2 + n_m,)),
            sem((2,)), sem((n_m, 2)), sem((2,)), sem((n_m,)),
            sem((PARTS,)), sem((1,)), sem((3 + 3 * n_m,)),
            pltpu.SemaphoreType.REGULAR((3,)),
        ],
        compiler_params=pltpu.CompilerParams(collective_id=0, has_side_effects=True, vmem_limit_bytes=34 * 2 ** 20),
        name='fused_update',
    )(g_in, g_out, w_in, w_out, m_in, m_out, r_in, c_in, r_out, c_out, lr.reshape(1), wd.reshape(1), b2.reshape(1))
    return tuple(pl.pallas_call(
        store_kernel,
        out_shape=tuple(jax.ShapeDtypeStruct(a.shape, a.dtype) for a in outs),
        in_specs=[vmem] * 8,
        out_specs=[hbm] * 8,
        scratch_shapes=[sem((8,))],
        compiler_params=pltpu.CompilerParams(vmem_limit_bytes=2 ** 20),
        name='store_out',
    )(*res))


def solution(mesh):
    in_specs = (P(None, None, 'tp'), P(None, 'tp', None), P('dp', None, None, 'tp'), P('dp', None, 'tp', None), P(None, 'dp', 'tp'), P(None, 'tp', 'dp'), P(None, 'dp'), P(None, 'tp'), P(None, 'tp'), P(None, 'dp'), P(), P(), P())
    out_specs = (P(None, None, 'tp'), P(None, 'tp', None), P(None, 'dp', 'tp'), P(None, 'tp', 'dp'), P(None, 'dp'), P(None, 'tp'), P(None, 'tp'), P(None, 'dp'))
    return jax.shard_map(local_step, mesh=mesh, in_specs=in_specs, out_specs=out_specs, check_vma=False)
```
